8 devices in a mesh: dp: 2 (over z, y), sp: 4 (over x, core).
Axes of the slice: x: 2, y: 2, z: 1, core: 2. Of those that a mesh axis runs over, the one named last changes fastest.
Arguments:
- hidden: bfloat16 [32, 1024, 768], P('dp', 'sp'), parts along dimension 0
- pos_ids: int32 [32, 1024], P('dp', 'sp'), parts along dimension 0
- block_ids: int32 [32, 1024], P('dp', 'sp'), parts along dimension 0
- ctx_len: int32 [32], P('dp'), parts along dimension 0
- ln_gamma: bfloat16 [768], replicated
- ln_beta: bfloat16 [768], replicated
- w_qkv: bfloat16 [768, 12, 3, 64], replicated
- b_qkv: bfloat16 [12, 3, 64], replicated
- w_dense: bfloat16 [768, 768], replicated
- b_dense: bfloat16 [768], replicated
Outputs:
- output 1: bfloat16 [32, 1024, 768], P('dp', 'sp'), parts along dimension 0
- output 2: bfloat16 [32, 1024, 12, 64], P('dp', None, 'sp'), parts along dimension 0
- output 3: bfloat16 [32, 1024, 12, 64], P('dp', None, 'sp'), parts along dimension 0
There are 2 independent parts. The reference program is written for one: setup_inputs(seed, part) draws one part's arguments, and reference() takes and returns one part's arrays. A program takes and returns all parts, laid end to end along the dimension named above; an argument that names none is the same for every part.
All inputs are finite; a program needn't handle non-finite values.
Results may differ from the reference program's by a relative error of at most 0.00593733.
Values are sent between devices in bfloat16 or wider.
A program may use at most 1 GiB of HBM per device.

```python
import math
import jax
import jax.numpy as jnp
from jax import lax

BATCH = 16
SEQ = 1024
HEADS = 12
HEAD = 64
HIDDEN = HEADS * HEAD
ALPHA = math.sqrt(56.0)
ROPE_BASE = 10000.0
LN_EPS = 1e-5
SCORE_SCALE = 1.0 / math.sqrt(HEAD)
QUERY_BLOCK = min(SEQ, 128)
GAIN = 1.0 / ALPHA
QKV_SCALE = ALPHA / math.sqrt(HIDDEN)
DENSE_SCALE = 0.5 * math.sqrt(SEQ / HIDDEN)
BIAS_SCALE = 1.0 / math.sqrt(SEQ)


def draw_positions(ctx_key, mask_key):
    ctx_len = jax.random.randint(ctx_key, (BATCH,), SEQ // 4, 3 * SEQ // 4 + 1, dtype=jnp.int32)
    mask_pos = jax.random.randint(mask_key, (BATCH,), 0, ctx_len, dtype=jnp.int32)
    token_pos = jnp.arange(SEQ, dtype=jnp.int32)[None, :]
    in_context = token_pos < ctx_len[:, None]
    pos_ids = jnp.where(in_context, token_pos, mask_pos[:, None]).astype(jnp.int32)
    block_ids = jnp.where(in_context, 0, token_pos - ctx_len[:, None] + 1).astype(jnp.int32)
    return pos_ids, block_ids, ctx_len


def setup_inputs(seed: int = 0, part: int = 0) -> dict:
    base_key = jax.random.key(seed)
    shared_key, part_key = jax.random.split(base_key)
    part_key = jax.random.fold_in(part_key, part)
    key_x, key_ctx, key_mask = jax.random.split(part_key, 3)
    key_g, key_b, key_w, key_wb, key_d, key_db = jax.random.split(shared_key, 6)
    pos_ids, block_ids, ctx_len = draw_positions(key_ctx, key_mask)
    hidden = jax.random.normal(key_x, (BATCH, SEQ, HIDDEN), jnp.float32)
    ln_gamma = (1.0 + 0.2 * jax.random.normal(key_g, (HIDDEN,), jnp.float32)) * GAIN
    ln_beta = jax.random.normal(key_b, (HIDDEN,), jnp.float32) * (GAIN * BIAS_SCALE)
    w_qkv = jax.random.normal(key_w, (HIDDEN, HEADS, 3, HEAD), jnp.float32) * QKV_SCALE
    b_qkv = jax.random.normal(key_wb, (HEADS, 3, HEAD), jnp.float32) * BIAS_SCALE
    w_dense = jax.random.normal(key_d, (HIDDEN, HIDDEN), jnp.float32) * DENSE_SCALE
    b_dense = jax.random.normal(key_db, (HIDDEN,), jnp.float32) * 0.5
    return {'hidden': hidden.astype(jnp.bfloat16), 'pos_ids': pos_ids, 'block_ids': block_ids, 'ctx_len': ctx_len, 'ln_gamma': ln_gamma.astype(jnp.bfloat16), 'ln_beta': ln_beta.astype(jnp.bfloat16), 'w_qkv': w_qkv.astype(jnp.bfloat16), 'b_qkv': b_qkv.astype(jnp.bfloat16), 'w_dense': w_dense.astype(jnp.bfloat16), 'b_dense': b_dense.astype(jnp.bfloat16)}


def layer_norm(hidden, ln_gamma, ln_beta):
    wide_in = hidden.astype(jnp.float32)
    row_mean = jnp.mean(wide_in, axis=-1, keepdims=True)
    centered = wide_in - row_mean
    row_var = jnp.mean(jnp.square(centered), axis=-1, keepdims=True)
    return (centered * lax.rsqrt(row_var + LN_EPS) * ln_gamma.astype(jnp.float32) + ln_beta.astype(jnp.float32)).astype(jnp.bfloat16)


def rotate(heads_in, pos_ids, block_ids):
    half_dim = heads_in.shape[-1] // 2
    quarter_dim = half_dim // 2
    inv_freq = ROPE_BASE ** (-jnp.arange(0, half_dim, 2).astype(jnp.float32) / half_dim)
    angles = jnp.stack([pos_ids, block_ids], axis=-1).astype(jnp.float32)[..., None] * inv_freq
    cos_a = jnp.cos(angles)[:, :, None]
    sin_a = jnp.sin(angles)[:, :, None]
    split_dims = heads_in.astype(jnp.float32).reshape(heads_in.shape[:-1] + (2, 2, quarter_dim))
    low_part = split_dims[..., 0, :]
    high_part = split_dims[..., 1, :]
    new_low = low_part * cos_a - high_part * sin_a
    new_high = high_part * cos_a + low_part * sin_a
    return jnp.stack([new_low, new_high], axis=-2).reshape(heads_in.shape).astype(jnp.bfloat16)


def reference(hidden, pos_ids, block_ids, ctx_len, ln_gamma, ln_beta, w_qkv, b_qkv, w_dense, b_dense):
    normed = layer_norm(hidden, ln_gamma, ln_beta)
    qkv_flat = jnp.dot(normed.reshape(BATCH * SEQ, HIDDEN), w_qkv.reshape(HIDDEN, 3 * HIDDEN), preferred_element_type=jnp.float32)
    qkv_proj = (qkv_flat.reshape(BATCH, SEQ, HEADS, 3, HEAD) + b_qkv.astype(jnp.float32)).astype(jnp.bfloat16)
    query_rot = rotate(qkv_proj[:, :, :, 0], pos_ids, block_ids)
    key_rot = rotate(qkv_proj[:, :, :, 1], pos_ids, block_ids)
    value_heads = qkv_proj[:, :, :, 2]
    key_pos = jnp.arange(SEQ)
    ctx_visible = key_pos[None, None, :] < ctx_len[:, None, None]

    def one_head(head_args):
        q_head, k_head, v_head = head_args
        k_wide = k_head.astype(jnp.float32)
        v_wide = v_head.astype(jnp.float32)

        def one_block(block_idx):
            block_start = block_idx * QUERY_BLOCK
            q_block = lax.dynamic_slice_in_dim(q_head, block_start, QUERY_BLOCK, axis=1).astype(jnp.float32)
            scores = jnp.einsum('bqe,bke->bqk', q_block, k_wide) * SCORE_SCALE
            q_pos = block_start + jnp.arange(QUERY_BLOCK)
            visible = ctx_visible | (key_pos[None, None, :] <= q_pos[None, :, None])
            attn_probs = jax.nn.softmax(jnp.where(visible, scores, -jnp.inf), axis=-1).astype(jnp.bfloat16)
            return jnp.einsum('bqk,bke->bqe', attn_probs.astype(jnp.float32), v_wide).astype(jnp.bfloat16)

        blocks = lax.map(one_block, jnp.arange(SEQ // QUERY_BLOCK))
        return jnp.moveaxis(blocks, 0, 1).reshape(BATCH, SEQ, HEAD)

    head_major = (jnp.moveaxis(query_rot, 2, 0), jnp.moveaxis(key_rot, 2, 0), jnp.moveaxis(value_heads, 2, 0))
    context = lax.map(one_head, head_major)
    context = jnp.moveaxis(context, 0, 2).reshape(BATCH * SEQ, HIDDEN)
    dense_out = jnp.dot(context, w_dense, preferred_element_type=jnp.float32) + b_dense.astype(jnp.float32)
    block_out = (normed.reshape(BATCH * SEQ, HIDDEN).astype(jnp.float32) * ALPHA + dense_out).astype(jnp.bfloat16)
    return block_out.reshape(BATCH, SEQ, HIDDEN), key_rot, value_heads
```

```python
import functools
import math
import numpy as np
import jax
import jax.numpy as jnp
from jax import lax
from jax.experimental import pallas as pl
from jax.experimental.pallas import tpu as pltpu
from jax.sharding import PartitionSpec as P

ALPHA = math.sqrt(56.0)
ROPE_BASE = 10000.0
LN_EPS = 1e-5
LOG2E = 1.4426950408889634
CHUNKS = (1, 2, 2, 2, 2, 2, 2, 2, 1)
F32 = jnp.float32
BF16 = jnp.bfloat16


def mm(a, b):
    return jnp.dot(a, b, preferred_element_type=F32)


def norm_kernel(h_ref, g_ref, b_ref, o_ref):
    x = h_ref[0].astype(F32)
    mean = jnp.mean(x, axis=-1, keepdims=True)
    x = x - mean
    var = jnp.mean(x * x, axis=-1, keepdims=True)
    y = x * lax.rsqrt(var + LN_EPS) * g_ref[...] + b_ref[...]
    o_ref[0] = y.astype(BF16).T


def rotate(x, tab):
    parts = []
    for half in range(2):
        u = x[32 * half:32 * half + 16]
        w = x[32 * half + 16:32 * half + 32]
        c = tab[32 * half:32 * half + 16]
        s = tab[32 * half + 16:32 * half + 32]
        parts.append(u * c - w * s)
        parts.append(w * c + u * s)
    return jnp.concatenate(parts, axis=0).astype(BF16)


def attn_kernel(heads, row0, idx_ref, ctx_ref, a0, a1, a2, a3, tab_ref, w_ref, bias_ref, *rest):
    rest = rest[-11:]
    k_out, v_out, c_own, c_send, kn, kt, vt, qt, s_s, p_s, dummy = rest
    hd = 64
    rows = heads * hd
    blk = a0.shape[2]
    ctx = ctx_ref[row0 + pl.program_id(0)]

    for m, a_ref in enumerate((a0, a1, a2, a3)):
        j = idx_ref[m]
        a = a_ref[0]
        tab = tab_ref[0, m]

        def project(part):
            lo = part * rows
            b = bias_ref[lo:lo + rows]
            return (mm(w_ref[lo:lo + rows], a) + jnp.concatenate([b, b], axis=1)).astype(BF16)

        if m < 2:
            q = project(0)
            for h in range(heads):
                qh = rotate(q[h * hd:(h + 1) * hd].astype(F32), tab)
                zero = jnp.zeros_like(qh)
                qt[m, h] = jnp.concatenate([qh, zero] if h % 2 == 0 else [zero, qh], axis=0)
        k = project(1)
        for p in range(heads // 2):
            pair = [rotate(k[(2 * p + i) * hd:(2 * p + i + 1) * hd].astype(F32), tab) for i in range(2)]
            pair = jnp.concatenate(pair, axis=0)
            kt[j, p * 128:(p + 1) * 128] = pair
            kn[j, p] = pair.T
        vt[j] = project(2)

    half = rows // 2
    out_lo = pl.multiple_of(idx_ref[4] * half, half)
    for j in range(4):
        k_out[0, :, j * blk:(j + 1) * blk] = kt[j, pl.ds(out_lo, half)]
        v_out[0, :, j * blk:(j + 1) * blk] = vt[j, pl.ds(out_lo, half)]

    scale = LOG2E / math.sqrt(hd)
    for qi, c_ref in enumerate((c_own, c_send)):
        jq = idx_ref[qi]
        blocks = jnp.maximum(jq + 1, (ctx + (blk - 1)) >> 8)

        def attend(nb):
            q_pos = jq * blk + lax.broadcasted_iota(jnp.int32, (1, blk), 1)
            limit = jnp.maximum(q_pos, ctx - 1)
            key_pos = (nb - 1) * blk + lax.broadcasted_iota(jnp.int32, (blk, blk), 0)

            def pair_step(p, carry):
                for i in range(2):
                    h = 2 * p + i
                    q = qt[qi, h]
                    top = None
                    for kb in range(nb):
                        s = mm(kn[kb, p], q)
                        if kb == nb - 1:
                            s = jnp.where(key_pos <= limit, s, -jnp.inf)
                        s_s[i, kb * blk:(kb + 1) * blk] = s
                        t = jnp.max(s, axis=0, keepdims=True)
                        top = t if top is None else jnp.maximum(top, t)
                    total = None
                    o = None
                    lo = pl.multiple_of(h * hd, hd)
                    for kb in range(nb):
                        e = jnp.exp2((s_s[i, kb * blk:(kb + 1) * blk] - top) * scale)
                        t = jnp.sum(e, axis=0, keepdims=True)
                        total = t if total is None else total + t
                        p_s[i, kb * blk:(kb + 1) * blk] = e.astype(BF16)
                    for kb in range(nb):
                        t = mm(vt[kb, pl.ds(lo, hd)], p_s[i, kb * blk:(kb + 1) * blk])
                        o = t if o is None else o + t
                    c_ref[0, pl.ds(lo, hd)] = (o / total).astype(BF16)
                return carry

            lax.fori_loop(0, heads // 2, pair_step, 0)

        for nb in (2, 3, 4):
            cond = blocks <= 2 if nb == 2 else blocks == nb
            pl.when(cond)(functools.partial(attend, nb))


def dense_kernel(own_ref, other_ref, a_ref, w_ref, b_ref, *rest):
    o_ref = rest[-1]
    half = own_ref.shape[1]
    acc = mm(w_ref[:, :half], own_ref[0]) + mm(w_ref[:, half:], other_ref[0])
    b = b_ref[...]
    acc = acc + a_ref[0].astype(F32) * ALPHA + jnp.concatenate([b, b], axis=1)
    o_ref[0] = acc.astype(BF16).T


def params(**kw):
    return pltpu.CompilerParams(dimension_semantics=("arbitrary",), vmem_limit_bytes=56 * 1024 * 1024, **kw)


def solution(mesh):
    seq_spec = P('dp', 'sp', None)
    row_spec = P('dp', 'sp')
    head_spec = P('dp', None, 'sp', None)
    replicated = P()
    across_x = [(i, i ^ 2) for i in range(4)]
    across_core = [(i, i ^ 1) for i in range(4)]

    def local_block(hidden, pos_ids, block_ids, ctx_len, ln_gamma, ln_beta, w_qkv, b_qkv, w_dense, b_dense):
        n_rows, blk, width = hidden.shape
        n_heads, _, hd = b_qkv.shape
        heads = n_heads // 2
        rows = heads * hd
        t = lax.axis_index('sp').astype(jnp.int32)
        core = t % 2
        idx = jnp.stack([t, t ^ 1, t ^ 2, t ^ 3, t // 2])
        gamma = ln_gamma.astype(F32)[None]
        beta = ln_beta.astype(F32)[None]

        starts = np.concatenate([[0], np.cumsum(CHUNKS)]).tolist()
        a_own, a_x, a_c, a_xc = [], [], [], []
        for i, n in enumerate(CHUNKS):
            r0 = starts[i]
            a = pl.pallas_call(
                norm_kernel,
                grid=(n,),
                in_specs=[pl.BlockSpec((1, blk, width), lambda b, r0=r0: (r0 + b, 0, 0)),
                          pl.BlockSpec((1, width), lambda b: (0, 0)),
                          pl.BlockSpec((1, width), lambda b: (0, 0))],
                out_specs=pl.BlockSpec((1, width, blk), lambda b: (b, 0, 0)),
                out_shape=jax.ShapeDtypeStruct((n, width, blk), BF16),
                compiler_params=params(),
                cost_estimate=pl.CostEstimate(flops=n * 300_000_000, bytes_accessed=n * 800_000, transcendentals=0),
                name="norm",
            )(hidden, gamma, beta)
            a_own.append(a)
            a_x.append(lax.ppermute(a, 'sp', across_x))
            a_c.append(lax.ppermute(a, 'sp', across_core))
        for i in range(len(CHUNKS)):
            a_xc.append(lax.ppermute(a_x[i], 'sp', across_core))

        ids = jnp.stack([pos_ids, block_ids], axis=1)
        ids_x = lax.ppermute(ids, 'sp', across_x)
        ids_c = lax.ppermute(ids, 'sp', across_core)
        ids_xc = lax.ppermute(ids_x, 'sp', across_core)
        inv_freq = jnp.asarray((ROPE_BASE ** (-np.arange(0, 32, 2, dtype=np.float64) / 32)).astype(np.float32))
        where = jnp.stack([ids, ids_c, ids_x, ids_xc], axis=1).astype(F32)
        angle = where[:, :, :, None, :] * inv_freq[None, None, None, :, None]
        tab = jnp.stack([jnp.cos(angle), jnp.sin(angle)], axis=3).reshape(n_rows, 4, 64, blk)

        w = w_qkv.transpose(2, 1, 3, 0).reshape(3, 2, 2, rows // 2, width)
        w = lax.dynamic_index_in_dim(w, core, 2, keepdims=False).reshape(3 * rows, width)
        bias = b_qkv.transpose(1, 0, 2).reshape(3, 2, 2, rows // 2)
        bias = lax.dynamic_index_in_dim(bias, core, 2, keepdims=False).reshape(3 * rows, 1)
        bias = jnp.broadcast_to(bias.astype(F32), (3 * rows, 128))
        wd = w_dense.T.reshape(width, 2, 2, rows // 2)
        wd_own = lax.dynamic_index_in_dim(wd, core, 2, keepdims=False).reshape(width, rows)
        wd_other = lax.dynamic_index_in_dim(wd, 1 - core, 2, keepdims=False).reshape(width, rows)
        wd = jnp.concatenate([wd_own, wd_other], axis=1)
        bd = jnp.broadcast_to(b_dense.astype(F32)[:, None], (width, 128))

        keys = values = out = None
        pending = []

        def finish(item, out):
            i, own, other = item
            n, r0 = CHUNKS[i], starts[i]
            extra = [] if out is None else [out]
            return pl.pallas_call(
                dense_kernel,
                grid=(n,),
                in_specs=[pl.BlockSpec((1, rows, blk), lambda b: (b, 0, 0)),
                          pl.BlockSpec((1, rows, blk), lambda b: (b, 0, 0)),
                          pl.BlockSpec((1, width, blk), lambda b: (b, 0, 0)),
                          pl.BlockSpec((width, width), lambda b: (0, 0)),
                          pl.BlockSpec((width, 128), lambda b: (0, 0))]
                + [pl.BlockSpec(memory_space=pl.ANY)] * len(extra),
                out_specs=pl.BlockSpec((1, blk, width), lambda b, r0=r0: (r0 + b, 0, 0)),
                out_shape=jax.ShapeDtypeStruct((n_rows, blk, width), BF16),
                input_output_aliases={5: 0} if extra else {},
                compiler_params=params(),
                cost_estimate=pl.CostEstimate(flops=n * 300_000_000, bytes_accessed=n * 2_000_000, transcendentals=0),
                name="dense",
            )(own, other, a_own[i], wd, bd, *extra)

        for i, n in enumerate(CHUNKS):
            r0 = starts[i]
            extra = [] if keys is None else [keys, values]
            a_spec = pl.BlockSpec((1, width, blk), lambda b, *_: (b, 0, 0))
            kv_shape = jax.ShapeDtypeStruct((n_rows, rows // 2, 4 * blk), BF16)
            kv_spec = pl.BlockSpec((1, rows // 2, 4 * blk), lambda b, *_, r0=r0: (r0 + b, 0, 0))
            c_shape = jax.ShapeDtypeStruct((n, rows, blk), BF16)
            c_spec = pl.BlockSpec((1, rows, blk), lambda b, *_: (b, 0, 0))
            keys, values, own, send = pl.pallas_call(
                functools.partial(attn_kernel, heads, r0),
                grid_spec=pltpu.PrefetchScalarGridSpec(
                    num_scalar_prefetch=2,
                    grid=(n,),
                    in_specs=[a_spec] * 4 + [
                        pl.BlockSpec((1, 4, 64, blk), lambda b, *_, r0=r0: (r0 + b, 0, 0, 0)),
                        pl.BlockSpec((3 * rows, width), lambda b, *_: (0, 0)),
                        pl.BlockSpec((3 * rows, 128), lambda b, *_: (0, 0))]
                    + [pl.BlockSpec(memory_space=pl.ANY)] * len(extra),
                    out_specs=[kv_spec, kv_spec, c_spec, c_spec],
                    scratch_shapes=[
                        pltpu.VMEM((4, heads // 2, blk, 128), BF16),
                        pltpu.VMEM((4, rows, blk), BF16),
                        pltpu.VMEM((4, rows, blk), BF16),
                        pltpu.VMEM((2, heads, 128, blk), BF16),
                        pltpu.VMEM((2, 4 * blk, blk), F32),
                        pltpu.VMEM((2, 4 * blk, blk), BF16),
                        pltpu.SMEM((1,), jnp.int32),
                    ],
                ),
                out_shape=[kv_shape, kv_shape, c_shape, c_shape],
                input_output_aliases={9: 0, 10: 1} if extra else {},
                compiler_params=params(),
                cost_estimate=pl.CostEstimate(flops=n * 6_000_000_000, bytes_accessed=n * 4_000_000, transcendentals=0),
                name="attn",
            )(idx, ctx_len, a_own[i], a_c[i], a_x[i], a_xc[i], tab, w, bias, *extra)
            other = lax.ppermute(send, 'sp', across_core)
            for item in pending:
                out = finish(item, out)
            pending = [(i, own, other)]
        for item in pending:
            out = finish(item, out)

        def by_heads(x):
            return x.reshape(n_rows, n_heads // 4, hd, 4 * blk).transpose(0, 3, 1, 2)

        return out, by_heads(keys), by_heads(values)

    return jax.shard_map(local_block, mesh=mesh, in_specs=(seq_spec, row_spec, row_spec, P('dp'), replicated, replicated, replicated, replicated, replicated, replicated), out_specs=(seq_spec, head_spec, head_spec), check_vma=False)
```

```python
import functools
import math
import numpy as np
import jax
import jax.numpy as jnp
from jax import lax
from jax.experimental import pallas as pl
from jax.experimental.pallas import tpu as pltpu
from jax.sharding import PartitionSpec as P

ALPHA = math.sqrt(56.0)
ROPE_BASE = 10000.0
LN_EPS = 1e-5
LOG2E = 1.4426950408889634
CHUNKS = (2, 2, 2, 2, 2, 2, 2, 1, 1)
F32 = jnp.float32
BF16 = jnp.bfloat16


def mm(a, b):
    return jnp.dot(a, b, preferred_element_type=F32)


def norm_kernel(counts, h_ref, g_ref, b_ref, *o_refs):
    x = h_ref[0].astype(F32)
    mean = jnp.mean(x, axis=-1, keepdims=True)
    x = x - mean
    var = jnp.mean(x * x, axis=-1, keepdims=True)
    y = x * lax.rsqrt(var + LN_EPS) * g_ref[...].astype(F32) + b_ref[...].astype(F32)
    y = y.astype(BF16).T
    row = pl.program_id(0)
    lo = 0
    for n, o_ref in zip(counts, o_refs):
        @pl.when((row >= lo) & (row < lo + n))
        def _():
            o_ref[0] = y
        lo += n


def rotate(x, tab):
    parts = []
    for half in range(2):
        u = x[32 * half:32 * half + 16]
        w = x[32 * half + 16:32 * half + 32]
        c = tab[32 * half:32 * half + 16]
        s = tab[32 * half + 16:32 * half + 32]
        parts.append(u * c - w * s)
        parts.append(w * c + u * s)
    return jnp.concatenate(parts, axis=0).astype(BF16)


def fold(x, op):
    x = [x[8 * i:8 * i + 8] for i in range(x.shape[0] // 8)]
    while len(x) > 1:
        x = [op(x[2 * i], x[2 * i + 1]) for i in range(len(x) // 2)]
    return x[0]


def attn_kernel(heads, row0, idx_ref, ctx_ref, a0, a1, a2, a3, tab_ref, w_ref, bias_ref, *rest):
    k_out, v_out, c_own, c_send, kn, kt, vt, qt, s_s, p_s, c_s = rest[-11:]
    hd = 64
    rows = heads * hd
    blk = a0.shape[2]
    ctx = ctx_ref[row0 + pl.program_id(0)]

    for m, a_ref in enumerate((a0, a1, a2, a3)):
        j = idx_ref[m]
        a = a_ref[0]
        tab = tab_ref[0, m]

        def project(part):
            lo = part * rows
            b = bias_ref[lo:lo + rows]
            return (mm(w_ref[lo:lo + rows], a) + jnp.concatenate([b, b], axis=1)).astype(BF16)

        if m < 2:
            q = project(0)
            for h in range(heads):
                qh = rotate(q[h * hd:(h + 1) * hd].astype(F32), tab)
                zero = jnp.zeros_like(qh)
                qt[m, h] = jnp.concatenate([qh, zero] if h % 2 == 0 else [zero, qh], axis=0)
        k = project(1)
        for p in range(heads // 2):
            pair = [rotate(k[(2 * p + i) * hd:(2 * p + i + 1) * hd].astype(F32), tab) for i in range(2)]
            pair = jnp.concatenate(pair, axis=0)
            kt[j, p * 128:(p + 1) * 128] = pair
            kn[j, p] = pair.T
        vt[j] = project(2)

    half = rows // 2
    out_lo = pl.multiple_of(idx_ref[4] * half, half)
    for j in range(4):
        k_out[0, :, j * blk:(j + 1) * blk] = kt[j, pl.ds(out_lo, half)]
        v_out[0, :, j * blk:(j + 1) * blk] = vt[j, pl.ds(out_lo, half)]

    scale = LOG2E / math.sqrt(hd)

    def attend(nb, qi, jq):
        q_pos = jq * blk + lax.broadcasted_iota(jnp.int32, (1, blk), 1)
        limit = jnp.maximum(q_pos, ctx - 1)
        top, total, acc = {}, {}, {}
        for step in range(heads + 2):
            h0, h1, h2 = step, step - 1, step - 2
            if 0 <= h1 < heads:
                top[h1] = jnp.max(top[h1], axis=0, keepdims=True)
            for kb in range(nb):
                lo = kb * blk
                if h0 < heads:
                    s = mm(kn[kb, h0 // 2], qt[qi, h0])
                    if kb == nb - 1:
                        key_pos = lo + lax.broadcasted_iota(jnp.int32, (blk, blk), 0)
                        s = jnp.where(key_pos <= limit, s, -jnp.inf)
                    s_s[h0 % 2, lo:lo + blk] = s
                    t = fold(s, jnp.maximum)
                    top[h0] = jnp.maximum(top[h0], t) if kb else t
                if 0 <= h1 < heads:
                    e = jnp.exp2((s_s[h1 % 2, lo:lo + blk] - top[h1]) * scale)
                    t = fold(e, jnp.add)
                    total[h1] = total[h1] + t if kb else t
                    p_s[h1 % 2, lo:lo + blk] = e.astype(BF16)
                if 0 <= h2 < heads:
                    t = mm(vt[kb, h2 * hd:(h2 + 1) * hd], p_s[h2 % 2, lo:lo + blk])
                    acc[h2] = acc[h2] + t if kb else t
            if 0 <= h2 < heads:
                t = jnp.sum(total[h2], axis=0, keepdims=True)
                c_s[qi, h2 * hd:(h2 + 1) * hd] = (acc[h2] / t).astype(BF16)

    def query_block(qi, carry):
        jq = idx_ref[qi]
        blocks = jnp.maximum(jq + 1, (ctx + (blk - 1)) // blk)
        for nb in (2, 3, 4):
            cond = blocks <= 2 if nb == 2 else blocks == nb
            pl.when(cond)(functools.partial(attend, nb, qi, jq))
        return carry

    lax.fori_loop(0, 2, query_block, 0)
    c_own[0] = c_s[0]
    c_send[0] = c_s[1]


def dense_kernel(own_ref, other_ref, a_ref, w_ref, b_ref, *rest):
    o_ref = rest[-1]
    half = own_ref.shape[1]
    acc = mm(w_ref[:, :half], own_ref[0]) + mm(w_ref[:, half:], other_ref[0])
    b = b_ref[...]
    acc = acc + a_ref[0].astype(F32) * ALPHA + jnp.concatenate([b, b], axis=1)
    o_ref[0] = acc.astype(BF16).T


def params(mib):
    return pltpu.CompilerParams(dimension_semantics=("arbitrary",), vmem_limit_bytes=mib * 1024 * 1024)


def solution(mesh):
    seq_spec = P('dp', 'sp', None)
    row_spec = P('dp', 'sp')
    head_spec = P('dp', None, 'sp', None)
    replicated = P()
    across_x = [(i, i ^ 2) for i in range(4)]
    across_core = [(i, i ^ 1) for i in range(4)]

    def local_block(hidden, pos_ids, block_ids, ctx_len, ln_gamma, ln_beta, w_qkv, b_qkv, w_dense, b_dense):
        n_rows, blk, width = hidden.shape
        n_heads, _, hd = b_qkv.shape
        heads = n_heads // 2
        rows = heads * hd
        t = lax.axis_index('sp').astype(jnp.int32)
        core = t % 2
        idx = jnp.stack([t, t ^ 1, t ^ 2, t ^ 3, t // 2])
        gamma = ln_gamma.reshape(1, width)
        beta = ln_beta.reshape(1, width)

        starts = np.concatenate([[0], np.cumsum(CHUNKS)]).tolist()

        def norm(first, counts):
            def out_spec(lo, n):
                return pl.BlockSpec((1, width, blk), lambda b: (jnp.clip(b - lo, 0, n - 1), 0, 0))
            lows = np.concatenate([[0], np.cumsum(counts)]).tolist()
            return pl.pallas_call(
                functools.partial(norm_kernel, counts),
                grid=(sum(counts),),
                in_specs=[pl.BlockSpec((1, blk, width), lambda b: (first + b, 0, 0)),
                          pl.BlockSpec((1, width), lambda b: (0, 0)),
                          pl.BlockSpec((1, width), lambda b: (0, 0))],
                out_specs=[out_spec(lo, n) for lo, n in zip(lows, counts)],
                out_shape=[jax.ShapeDtypeStruct((n, width, blk), BF16) for n in counts],
                compiler_params=params(60),
                cost_estimate=pl.CostEstimate(flops=sum(counts) * 500_000_000, bytes_accessed=sum(counts) * 800_000, transcendentals=0),
                name="norm",
            )(hidden, gamma, beta)

        a_own = norm(0, CHUNKS[:1])
        a_x = [lax.ppermute(a_own[0], 'sp', across_x)]
        a_own = list(a_own) + list(norm(CHUNKS[0], CHUNKS[1:]))
        a_x += [lax.ppermute(a, 'sp', across_x) for a in a_own[1:]]

        ids = jnp.stack([pos_ids, block_ids], axis=1)
        ids_x = lax.ppermute(ids, 'sp', across_x)
        ids_c = lax.ppermute(ids, 'sp', across_core)
        ids_xc = lax.ppermute(ids_x, 'sp', across_core)
        inv_freq = jnp.asarray((ROPE_BASE ** (-np.arange(0, 32, 2, dtype=np.float64) / 32)).astype(np.float32))
        where = jnp.stack([ids, ids_c, ids_x, ids_xc], axis=1).astype(F32)
        angle = where[:, :, :, None, :] * inv_freq[None, None, None, :, None]
        tab = jnp.stack([jnp.cos(angle), jnp.sin(angle)], axis=3).reshape(n_rows, 4, 64, blk)

        w = w_qkv.transpose(2, 1, 3, 0).reshape(3, 2, 2, rows // 2, width)
        w = lax.dynamic_index_in_dim(w, core, 2, keepdims=False).reshape(3 * rows, width)
        bias = b_qkv.transpose(1, 0, 2).reshape(3, 2, 2, rows // 2)
        bias = lax.dynamic_index_in_dim(bias, core, 2, keepdims=False).reshape(3 * rows, 1)
        bias = jnp.broadcast_to(bias.astype(F32), (3 * rows, 128))
        wd = w_dense.T.reshape(width, 2, 2, rows // 2)
        wd_own = lax.dynamic_index_in_dim(wd, core, 2, keepdims=False).reshape(width, rows)
        wd_other = lax.dynamic_index_in_dim(wd, 1 - core, 2, keepdims=False).reshape(width, rows)
        wd = jnp.concatenate([wd_own, wd_other], axis=1)
        bd = jnp.broadcast_to(b_dense.astype(F32)[:, None], (width, 128))

        keys = values = out = None
        pending = []

        def finish(item, out):
            i, own, other = item
            n, r0 = CHUNKS[i], starts[i]
            extra = [] if out is None else [out]
            return pl.pallas_call(
                dense_kernel,
                grid=(n,),
                in_specs=[pl.BlockSpec((1, rows, blk), lambda b: (b, 0, 0)),
                          pl.BlockSpec((1, rows, blk), lambda b: (b, 0, 0)),
                          pl.BlockSpec((1, width, blk), lambda b: (b, 0, 0)),
                          pl.BlockSpec((width, width), lambda b: (0, 0)),
                          pl.BlockSpec((width, 128), lambda b: (0, 0))]
                + [pl.BlockSpec(memory_space=pl.ANY)] * len(extra),
                out_specs=pl.BlockSpec((1, blk, width), lambda b, r0=r0: (r0 + b, 0, 0)),
                out_shape=jax.ShapeDtypeStruct((n_rows, blk, width), BF16),
                input_output_aliases={5: 0} if extra else {},
                compiler_params=params(16),
                cost_estimate=pl.CostEstimate(flops=n * 1_000_000_000, bytes_accessed=n * 2_000_000, transcendentals=0),
                name="dense",
            )(own, other, a_own[i], wd, bd, *extra)

        a_c, a_xc = {}, {}

        def fetch(i, after):
            got = lax.optimization_barrier((a_own[i], a_x[i], *after))
            a_c[i] = lax.ppermute(got[0], 'sp', across_core)
            a_xc[i] = lax.ppermute(got[1], 'sp', across_core)

        fetch(0, ())
        for i, n in enumerate(CHUNKS):
            r0 = starts[i]
            extra = [] if keys is None else [keys, values]
            a_spec = pl.BlockSpec((1, width, blk), lambda b, *_: (b, 0, 0))
            kv_shape = jax.ShapeDtypeStruct((n_rows, rows // 2, 4 * blk), BF16)
            kv_spec = pl.BlockSpec((1, rows // 2, 4 * blk), lambda b, *_, r0=r0: (r0 + b, 0, 0))
            c_shape = jax.ShapeDtypeStruct((n, rows, blk), BF16)
            c_spec = pl.BlockSpec((1, rows, blk), lambda b, *_: (b, 0, 0))
            keys, values, own, send = pl.pallas_call(
                functools.partial(attn_kernel, heads, r0),
                grid_spec=pltpu.PrefetchScalarGridSpec(
                    num_scalar_prefetch=2,
                    grid=(n,),
                    in_specs=[a_spec] * 4 + [
                        pl.BlockSpec((1, 4, 64, blk), lambda b, *_, r0=r0: (r0 + b, 0, 0, 0)),
                        pl.BlockSpec((3 * rows, width), lambda b, *_: (0, 0)),
                        pl.BlockSpec((3 * rows, 128), lambda b, *_: (0, 0))]
                    + [pl.BlockSpec(memory_space=pl.ANY)] * len(extra),
                    out_specs=[kv_spec, kv_spec, c_spec, c_spec],
                    scratch_shapes=[
                        pltpu.VMEM((4, heads // 2, blk, 128), BF16),
                        pltpu.VMEM((4, rows, blk), BF16),
                        pltpu.VMEM((4, rows, blk), BF16),
                        pltpu.VMEM((2, heads, 128, blk), BF16),
                        pltpu.VMEM((2, 4 * blk, blk), F32),
                        pltpu.VMEM((2, 4 * blk, blk), BF16),
                        pltpu.VMEM((2, rows, blk), BF16),
                    ],
                ),
                out_shape=[kv_shape, kv_shape, c_shape, c_shape],
                input_output_aliases={9: 0, 10: 1} if extra else {},
                compiler_params=params(32),
                cost_estimate=pl.CostEstimate(flops=n * 6_000_000_000, bytes_accessed=n * 4_000_000, transcendentals=0),
                name="attn",
            )(idx, ctx_len, a_own[i], a_c[i], a_x[i], a_xc[i], tab, w, bias, *extra)
            other = lax.ppermute(send, 'sp', across_core)
            if i + 1 < len(CHUNKS):
                fetch(i + 1, (own,) + (() if out is None else (out,)))
            for item in pending:
                out = finish(item, out)
            pending = [(i, own, other)]
        for item in pending:
            out = finish(item, out)

        def by_heads(x):
            return x.reshape(n_rows, n_heads // 4, hd, 4 * blk).transpose(0, 3, 1, 2)

        return out, by_heads(keys), by_heads(values)

    return jax.shard_map(local_block, mesh=mesh, in_specs=(seq_spec, row_spec, row_spec, P('dp'), replicated, replicated, replicated, replicated, replicated, replicated), out_specs=(seq_spec, head_spec, head_spec), check_vma=False)
```

```python
import functools
import math
import numpy as np
import jax
import jax.numpy as jnp
from jax import lax
from jax.experimental import pallas as pl
from jax.experimental.pallas import tpu as pltpu
from jax.sharding import PartitionSpec as P

ALPHA = math.sqrt(56.0)
ROPE_BASE = 10000.0
LN_EPS = 1e-5
LOG2E = 1.4426950408889634
CHUNKS = (2, 2, 2, 2, 2, 2, 2, 1, 1)
F32 = jnp.float32
BF16 = jnp.bfloat16


def mm(a, b):
    return jnp.dot(a, b, preferred_element_type=F32)


def row_vector(ref):
    return ref[...].astype(F32).reshape(1, ref.shape[0])


def norm_kernel(plan, h_ref, g_ref, b_ref, *o_refs):
    def row(r):
        x = h_ref[r].astype(F32)
        x = x - jnp.mean(x, axis=-1, keepdims=True)
        var = jnp.mean(x * x, axis=-1, keepdims=True)
        y = x * lax.rsqrt(var + LN_EPS) * row_vector(g_ref) + row_vector(b_ref)
        return y.astype(BF16).T

    out = [row(r) for r in range(h_ref.shape[0])]
    step = pl.program_id(0)
    for (lo, hi, rows), o_ref in zip(plan, o_refs):
        @pl.when((step >= lo) & (step <= hi))
        def _():
            for i, r in enumerate(rows):
                o_ref[i] = out[r]


def rotate(x, cos_a, sin_a, cos_b, sin_b):
    u0, w0, u1, w1 = (x[16 * i:16 * i + 16] for i in range(4))
    parts = [u0 * cos_a - w0 * sin_a, w0 * cos_a + u0 * sin_a,
             u1 * cos_b - w1 * sin_b, w1 * cos_b + u1 * sin_b]
    return jnp.concatenate(parts, axis=0).astype(BF16)


def fold(accs, x, op):
    accs = list(accs) if accs else [None] * 4
    for i in range(x.shape[0] // 8):
        v = x[8 * i:8 * i + 8]
        accs[i % 4] = v if accs[i % 4] is None else op(accs[i % 4], v)
    return accs


def join(accs, op):
    return op(op(accs[0], accs[1]), op(accs[2], accs[3]))


def attn_kernel(heads, row0, idx_ref, ctx_ref, a0, a1, a2, a3, tab_ref, col_ref, w_ref, bias_ref, *rest):
    k_out, v_out, c_own, c_send, kn, kt, vt, qt, s_s, p_s, c_s, m_s = rest[-12:]
    hd = 64
    rows = heads * hd
    blk = a0.shape[2]
    ctx = ctx_ref[row0 + pl.program_id(0)]

    col = [jnp.concatenate([col_ref[0, 16 * i:16 * i + 16]] * 2, axis=1) for i in range(4)]
    for m, a_ref in enumerate((a0, a1, a2, a3)):
        j = idx_ref[m]
        a = a_ref[0]
        cos, sin = tab_ref[j, :16], tab_ref[j, 16:]
        inside = j * blk + lax.broadcasted_iota(jnp.int32, (1, blk), 1) < ctx
        tab = (jnp.where(inside, cos, col[0]), jnp.where(inside, sin, col[1]),
               jnp.where(inside, 1.0, cos * col[2] + sin * col[3]),
               jnp.where(inside, 0.0, sin * col[2] - cos * col[3]))

        def project(part):
            lo = part * rows
            b = bias_ref[lo:lo + rows]
            return (mm(w_ref[lo:lo + rows], a) + jnp.concatenate([b, b], axis=1)).astype(BF16)

        if m < 2:
            q = project(0)
            for h in range(heads):
                qh = rotate(q[h * hd:(h + 1) * hd].astype(F32), *tab)
                zero = jnp.zeros_like(qh)
                qt[m, h] = jnp.concatenate([qh, zero] if h % 2 == 0 else [zero, qh], axis=0)
        k = project(1)
        for p in range(heads // 2):
            pair = [rotate(k[(2 * p + i) * hd:(2 * p + i + 1) * hd].astype(F32), *tab) for i in range(2)]
            pair = jnp.concatenate(pair, axis=0)
            kt[j, p * 128:(p + 1) * 128] = pair
            kn[j, p] = pair.T
        vt[j] = project(2)

    half = rows // 2
    out_lo = pl.multiple_of(idx_ref[4] * half, half)
    for j in range(4):
        k_out[0, :, j * blk:(j + 1) * blk] = kt[j, pl.ds(out_lo, half)]
        v_out[0, :, j * blk:(j + 1) * blk] = vt[j, pl.ds(out_lo, half)]

    scale = LOG2E / math.sqrt(hd)

    def attend(nb, masked, qi, jq):
        q_pos = jq * blk + lax.broadcasted_iota(jnp.int32, (1, blk), 1)
        limit = jnp.maximum(q_pos, ctx - 1)
        for kb in masked:
            key_pos = kb * blk + lax.broadcasted_iota(jnp.int32, (blk, blk), 0)
            m_s[kb % 2] = jnp.where(key_pos <= limit, 0.0, -jnp.inf)
        top, total, acc = {}, {}, {}
        for step in range(heads + 2):
            h0, h1, h2 = step, step - 1, step - 2
            if 0 <= h1 < heads:
                top[h1] = jnp.max(join(top[h1], jnp.maximum), axis=0, keepdims=True)
            for kb in range(nb):
                lo = kb * blk
                if h0 < heads:
                    s = mm(kn[kb, h0 // 2], qt[qi, h0])
                    if kb in masked:
                        s = s + m_s[kb % 2]
                    s_s[h0 % 2, lo:lo + blk] = s
                    top[h0] = fold(top.get(h0), s, jnp.maximum)
                if 0 <= h1 < heads:
                    for r in range(lo, lo + blk, 32):
                        e = jnp.exp2((s_s[h1 % 2, r:r + 32] - top[h1]) * scale)
                        total[h1] = fold(total.get(h1), e, jnp.add)
                        p_s[h1 % 2, r:r + 32] = e.astype(BF16)
                if 0 <= h2 < heads:
                    t = mm(vt[kb, h2 * hd:(h2 + 1) * hd], p_s[h2 % 2, lo:lo + blk])
                    acc[h2] = acc[h2] + t if kb else t
            if 0 <= h2 < heads:
                t = jnp.sum(join(total[h2], jnp.add), axis=0, keepdims=True)
                c_s[qi, h2 * hd:(h2 + 1) * hd] = (acc[h2] / t).astype(BF16)

    def query_block(qi, carry):
        jq = idx_ref[qi]
        pl.when(jq < 3)(functools.partial(attend, 3, (1, 2), qi, jq))
        pl.when(jq == 3)(functools.partial(attend, 4, (3,), qi, jq))
        return carry

    lax.fori_loop(0, 2, query_block, 0)
    c_own[0] = c_s[0].T
    c_send[0] = c_s[1].T


def dense_kernel(idx_ref, own_ref, other_ref, a_ref, w0, w1, w2, w3, b_ref, *rest):
    o_ref = rest[-1]
    for r in range(o_ref.shape[0]):
        w = jnp.concatenate([w0[0], w1[0]], axis=0)
        acc = mm(own_ref[r], w)
        w = jnp.concatenate([w2[0], w3[0]], axis=0)
        acc = acc + mm(other_ref[r], w)
        o_ref[r] = (a_ref[r].T.astype(F32) * ALPHA + (acc + row_vector(b_ref))).astype(BF16)


def params(mib):
    return pltpu.CompilerParams(dimension_semantics=("arbitrary",), vmem_limit_bytes=mib * 1024 * 1024)


def solution(mesh):
    seq_spec = P('dp', 'sp', None)
    row_spec = P('dp', 'sp')
    head_spec = P('dp', None, 'sp', None)
    replicated = P()
    across_x = [(i, i ^ 2) for i in range(4)]
    across_core = [(i, i ^ 1) for i in range(4)]
    inv_freq = ROPE_BASE ** (-np.arange(0, 32, 2, dtype=np.float64) / 32)

    def local_block(hidden, pos_ids, block_ids, ctx_len, ln_gamma, ln_beta, w_qkv, b_qkv, w_dense, b_dense):
        n_rows, blk, width = hidden.shape
        n_heads, _, hd = b_qkv.shape
        heads = n_heads // 2
        rows = heads * hd
        half = rows // 2
        t = lax.axis_index('sp').astype(jnp.int32)
        core = t & 1
        idx = jnp.stack([t, t ^ 1, t ^ 2, t ^ 3, t >> 1, core, 2 + core, 1 - core, 3 - core])
        starts = np.concatenate([[0], np.cumsum(CHUNKS)]).tolist()

        def norm(chunks):
            first = starts[chunks[0]]
            step_rows = 2 if all(starts[i] % 2 == 0 or CHUNKS[i] == 1 for i in chunks) else 1
            plan, specs, shapes = [], [], []
            for i in chunks:
                r0, r1 = starts[i] - first, starts[i + 1] - first
                lo, hi = r0 // step_rows, (r1 - 1) // step_rows
                n = min(step_rows, r1 - r0)
                plan.append((lo, hi, [(r0 + k) % step_rows for k in range(n)]))
                specs.append(pl.BlockSpec((n, width, blk), lambda b, lo=lo, hi=hi: (jnp.clip(b - lo, 0, hi - lo), 0, 0)))
                shapes.append(jax.ShapeDtypeStruct((r1 - r0, width, blk), BF16))
            total = starts[chunks[-1] + 1] - first
            return list(pl.pallas_call(
                functools.partial(norm_kernel, plan),
                grid=(total // step_rows,),
                in_specs=[pl.BlockSpec((step_rows, blk, width), lambda b: (first // step_rows + b, 0, 0)),
                          pl.BlockSpec((width,), lambda b: (0,)),
                          pl.BlockSpec((width,), lambda b: (0,))],
                out_specs=specs,
                out_shape=shapes,
                compiler_params=params(60),
                cost_estimate=pl.CostEstimate(flops=total * 500_000_000, bytes_accessed=total * 800_000, transcendentals=0),
                name="norm",
            )(hidden, ln_gamma, ln_beta))

        a_own = norm([0])
        a_x = [lax.ppermute(a_own[0], 'sp', across_x)]
        a_own += norm(list(range(1, len(CHUNKS))))
        a_x += [lax.ppermute(a, 'sp', across_x) for a in a_own[1:]]

        last = pos_ids[:, blk - 1:].reshape(1, n_rows)
        last_x = lax.ppermute(last, 'sp', across_x)
        last_c = lax.ppermute(last, 'sp', across_core)
        last_xc = lax.ppermute(last_x, 'sp', across_core)
        mask_pos = jnp.where(t == 3, last, jnp.where(t == 2, last_c, jnp.where(t == 1, last_x, last_xc)))[0]
        freq = jnp.asarray(inv_freq.astype(np.float32))
        angle = jnp.stack([mask_pos, ctx_len - 1], axis=1).astype(F32)[:, :, None] * freq
        col = jnp.stack([jnp.cos(angle), jnp.sin(angle)], axis=2).reshape(n_rows, 64, 1)
        col = jnp.broadcast_to(col, (n_rows, 64, 128))
        angle = inv_freq[None, :, None] * np.arange(4 * blk).reshape(4, 1, blk)
        tab = jnp.asarray(np.concatenate([np.cos(angle), np.sin(angle)], axis=1).astype(np.float32))

        w = w_qkv.transpose(2, 1, 3, 0).reshape(3, 2, 2, half, width)
        w = lax.dynamic_index_in_dim(w, core, 2, keepdims=False).reshape(3 * rows, width)
        bias = b_qkv.transpose(1, 0, 2).reshape(3, 2, 2, half)
        bias = lax.dynamic_index_in_dim(bias, core, 2, keepdims=False).reshape(3 * rows, 1)
        bias = jnp.broadcast_to(bias.astype(F32), (3 * rows, 128))
        wd = w_dense.reshape(4, half, width)

        keys = values = out = None

        def finish(item, out):
            i, own, other = item
            n, r0 = CHUNKS[i], starts[i]
            extra = [] if out is None else [out]
            return pl.pallas_call(
                dense_kernel,
                grid_spec=pltpu.PrefetchScalarGridSpec(
                    num_scalar_prefetch=1,
                    grid=(n,),
                    in_specs=[pl.BlockSpec((1, blk, rows), lambda b, s: (b, 0, 0)),
                              pl.BlockSpec((1, blk, rows), lambda b, s: (b, 0, 0)),
                              pl.BlockSpec((1, width, blk), lambda b, s: (b, 0, 0))]
                    + [pl.BlockSpec((1, half, width), lambda b, s, k=k: (s[k], 0, 0)) for k in (5, 6, 7, 8)]
                    + [pl.BlockSpec((width,), lambda b, s: (0,))]
                    + [pl.BlockSpec(memory_space=pl.ANY)] * len(extra),
                    out_specs=pl.BlockSpec((1, blk, width), lambda b, s: (r0 + b, 0, 0)),
                ),
                out_shape=jax.ShapeDtypeStruct((n_rows, blk, width), BF16),
                input_output_aliases={9: 0} if extra else {},
                compiler_params=params(24),
                cost_estimate=pl.CostEstimate(flops=n * 1_000_000_000, bytes_accessed=n * 2_000_000, transcendentals=0),
                name="dense",
            )(idx, own, other, a_own[i], wd, wd, wd, wd, b_dense, *extra)

        a_c, a_xc = {}, {}

        def fetch(i, after):
            got = lax.optimization_barrier((a_own[i], a_x[i], *after))
            a_c[i] = lax.ppermute(got[0], 'sp', across_core)
            a_xc[i] = lax.ppermute(got[1], 'sp', across_core)

        fetch(0, ())
        pending = []
        for i, n in enumerate(CHUNKS):
            r0 = starts[i]
            extra = [] if keys is None else [keys, values]
            a_spec = pl.BlockSpec((1, width, blk), lambda b, *_: (b, 0, 0))
            kv_shape = jax.ShapeDtypeStruct((n_rows, half, 4 * blk), BF16)
            kv_spec = pl.BlockSpec((1, half, 4 * blk), lambda b, *_, r0=r0: (r0 + b, 0, 0))
            c_shape = jax.ShapeDtypeStruct((n, blk, rows), BF16)
            c_spec = pl.BlockSpec((1, blk, rows), lambda b, *_: (b, 0, 0))
            keys, values, own, send = pl.pallas_call(
                functools.partial(attn_kernel, heads, r0),
                grid_spec=pltpu.PrefetchScalarGridSpec(
                    num_scalar_prefetch=2,
                    grid=(n,),
                    in_specs=[a_spec] * 4 + [
                        pl.BlockSpec((4, 32, blk), lambda b, *_: (0, 0, 0)),
                        pl.BlockSpec((1, 64, 128), lambda b, *_, r0=r0: (r0 + b, 0, 0)),
                        pl.BlockSpec((3 * rows, width), lambda b, *_: (0, 0)),
                        pl.BlockSpec((3 * rows, 128), lambda b, *_: (0, 0))]
                    + [pl.BlockSpec(memory_space=pl.ANY)] * len(extra),
                    out_specs=[kv_spec, kv_spec, c_spec, c_spec],
                    scratch_shapes=[
                        pltpu.VMEM((4, heads // 2, blk, 128), BF16),
                        pltpu.VMEM((4, rows, blk), BF16),
                        pltpu.VMEM((4, rows, blk), BF16),
                        pltpu.VMEM((2, heads, 128, blk), BF16),
                        pltpu.VMEM((2, 4 * blk, blk), F32),
                        pltpu.VMEM((2, 4 * blk, blk), BF16),
                        pltpu.VMEM((2, rows, blk), BF16),
                        pltpu.VMEM((2, blk, blk), F32),
                    ],
                ),
                out_shape=[kv_shape, kv_shape, c_shape, c_shape],
                input_output_aliases={10: 0, 11: 1} if extra else {},
                compiler_params=params(28),
                cost_estimate=pl.CostEstimate(flops=n * 6_000_000_000, bytes_accessed=n * 4_000_000, transcendentals=0),
                name="attn",
            )(idx, ctx_len, a_own[i], a_c[i], a_x[i], a_xc[i], tab, col, w, bias, *extra)
            other = lax.ppermute(send, 'sp', across_core)
            if i + 1 < len(CHUNKS):
                fetch(i + 1, (own,) + (() if out is None else (out,)))
            for item in pending:
                out = finish(item, out)
            pending = [(i, own, other)]
        for item in pending:
            out = finish(item, out)

        def by_heads(x):
            return x.reshape(n_rows, n_heads // 4, hd, 4 * blk).transpose(0, 3, 1, 2)

        return out, by_heads(keys), by_heads(values)

    return jax.shard_map(local_block, mesh=mesh, in_specs=(seq_spec, row_spec, row_spec, P('dp'), replicated, replicated, replicated, replicated, replicated, replicated), out_specs=(seq_spec, head_spec, head_spec), check_vma=False)
```

```python
import functools
import math
import numpy as np
import jax
import jax.numpy as jnp
from jax import lax
from jax.experimental import pallas as pl
from jax.experimental.pallas import tpu as pltpu
from jax.sharding import PartitionSpec as P

ALPHA = math.sqrt(56.0)
ROPE_BASE = 10000.0
LN_EPS = 1e-5
LOG2E = 1.4426950408889634
CHUNKS = (2, 3, 3, 3, 3, 2)
F32 = jnp.float32
BF16 = jnp.bfloat16


def mm(a, b):
    return jnp.dot(a, b, preferred_element_type=F32)


def row_vector(ref):
    return ref[...].astype(F32).reshape(1, ref.shape[0])


def norm_kernel(plan, h_ref, g_ref, b_ref, *o_refs):
    def row(r):
        x = h_ref[r].astype(F32)
        x = x - jnp.mean(x, axis=-1, keepdims=True)
        var = jnp.mean(x * x, axis=-1, keepdims=True)
        y = x * lax.rsqrt(var + LN_EPS) * row_vector(g_ref) + row_vector(b_ref)
        return y.astype(BF16).T

    out = [row(r) for r in range(h_ref.shape[0])]
    step = pl.program_id(0)
    for (lo, hi, rows), o_ref in zip(plan, o_refs):
        @pl.when((step >= lo) & (step <= hi))
        def _():
            for i, r in enumerate(rows):
                o_ref[i] = out[r]


def rotate(x, cos_a, sin_a, cos_b, sin_b):
    u0, w0, u1, w1 = (x[16 * i:16 * i + 16] for i in range(4))
    parts = [u0 * cos_a - w0 * sin_a, w0 * cos_a + u0 * sin_a,
             u1 * cos_b - w1 * sin_b, w1 * cos_b + u1 * sin_b]
    return jnp.concatenate(parts, axis=0).astype(BF16)


def fold(accs, x, op):
    accs = list(accs) if accs else [None] * 4
    for i in range(x.shape[0] // 8):
        v = x[8 * i:8 * i + 8]
        accs[i % 4] = v if accs[i % 4] is None else op(accs[i % 4], v)
    return accs


def join(accs, op):
    return op(op(accs[0], accs[1]), op(accs[2], accs[3]))


def attn_kernel(heads, row0, idx_ref, ctx_ref, a0, a1, a2, a3, tab_ref, col_ref, w_ref, bias_ref, *rest):
    k_out, v_out, c_own, c_send, kn, kt, vt, qt, s_s, p_s, c_s, m_s = rest[-12:]
    hd = 64
    rows = heads * hd
    blk = a0.shape[2]
    ctx = ctx_ref[row0 + pl.program_id(0)]

    col = [jnp.concatenate([col_ref[0, 16 * i:16 * i + 16]] * 2, axis=1) for i in range(4)]
    for m, a_ref in enumerate((a0, a1, a2, a3)):
        j = idx_ref[m]
        a = a_ref[0]
        cos, sin = tab_ref[j, :16], tab_ref[j, 16:]
        inside = j * blk + lax.broadcasted_iota(jnp.int32, (1, blk), 1) < ctx
        tab = (jnp.where(inside, cos, col[0]), jnp.where(inside, sin, col[1]),
               jnp.where(inside, 1.0, cos * col[2] + sin * col[3]),
               jnp.where(inside, 0.0, sin * col[2] - cos * col[3]))

        def project(part):
            lo = part * rows
            b = bias_ref[lo:lo + rows]
            return (mm(w_ref[lo:lo + rows], a) + jnp.concatenate([b, b], axis=1)).astype(BF16)

        if m < 2:
            q = project(0)
            for h in range(heads):
                qh = rotate(q[h * hd:(h + 1) * hd].astype(F32), *tab)
                zero = jnp.zeros_like(qh)
                qt[m, h] = jnp.concatenate([qh, zero] if h % 2 == 0 else [zero, qh], axis=0)
        k = project(1)
        for p in range(heads // 2):
            pair = [rotate(k[(2 * p + i) * hd:(2 * p + i + 1) * hd].astype(F32), *tab) for i in range(2)]
            pair = jnp.concatenate(pair, axis=0)
            kt[j, p * 128:(p + 1) * 128] = pair
            kn[j, p] = pair.T
        vt[j] = project(2)

    half = rows // 2
    out_lo = pl.multiple_of(idx_ref[4] * half, half)
    for j in range(4):
        k_out[0, :, j * blk:(j + 1) * blk] = kt[j, pl.ds(out_lo, half)]
        v_out[0, :, j * blk:(j + 1) * blk] = vt[j, pl.ds(out_lo, half)]

    scale = LOG2E / math.sqrt(hd)

    def attend(nb, masked, qi, jq):
        q_pos = jq * blk + lax.broadcasted_iota(jnp.int32, (1, blk), 1)
        limit = jnp.maximum(q_pos, ctx - 1)
        for kb in masked:
            key_pos = kb * blk + lax.broadcasted_iota(jnp.int32, (blk, blk), 0)
            m_s[kb % 2] = jnp.where(key_pos <= limit, 0.0, -jnp.inf)
        top, total, acc = {}, {}, {}
        for step in range(heads + 2):
            h0, h1, h2 = step, step - 1, step - 2
            if 0 <= h1 < heads:
                top[h1] = jnp.max(join(top[h1], jnp.maximum), axis=0, keepdims=True)
            for kb in range(nb):
                lo = kb * blk
                if h0 < heads:
                    s = mm(kn[kb, h0 // 2], qt[qi, h0])
                    if kb in masked:
                        s = s + m_s[kb % 2]
                    s_s[h0 % 2, lo:lo + blk] = s
                    top[h0] = fold(top.get(h0), s, jnp.maximum)
                if 0 <= h1 < heads:
                    for r in range(lo, lo + blk, 32):
                        e = jnp.exp2((s_s[h1 % 2, r:r + 32] - top[h1]) * scale)
                        total[h1] = fold(total.get(h1), e, jnp.add)
                        p_s[h1 % 2, r:r + 32] = e.astype(BF16)
                if 0 <= h2 < heads:
                    t = mm(vt[kb, h2 * hd:(h2 + 1) * hd], p_s[h2 % 2, lo:lo + blk])
                    acc[h2] = acc[h2] + t if kb else t
            if 0 <= h2 < heads:
                t = jnp.sum(join(total[h2], jnp.add), axis=0, keepdims=True)
                c_s[qi, h2 * hd:(h2 + 1) * hd] = (acc[h2] / t).astype(BF16)

    def query_block(qi, carry):
        jq = idx_ref[qi]
        pl.when(jq < 3)(functools.partial(attend, 3, (1, 2), qi, jq))
        pl.when(jq == 3)(functools.partial(attend, 4, (3,), qi, jq))
        return carry

    lax.fori_loop(0, 2, query_block, 0)
    c_own[0] = c_s[0].T
    c_send[0] = c_s[1].T


def dense_kernel(idx_ref, own_ref, other_ref, a_ref, w0, w1, w2, w3, b_ref, *rest):
    o_ref = rest[-1]
    for r in range(o_ref.shape[0]):
        w = jnp.concatenate([w0[0], w1[0]], axis=0)
        acc = mm(own_ref[r], w)
        w = jnp.concatenate([w2[0], w3[0]], axis=0)
        acc = acc + mm(other_ref[r], w)
        o_ref[r] = (a_ref[r].T.astype(F32) * ALPHA + (acc + row_vector(b_ref))).astype(BF16)


def params(mib):
    return pltpu.CompilerParams(dimension_semantics=("arbitrary",), vmem_limit_bytes=mib * 1024 * 1024)


def solution(mesh):
    seq_spec = P('dp', 'sp', None)
    row_spec = P('dp', 'sp')
    head_spec = P('dp', None, 'sp', None)
    replicated = P()
    across_x = [(i, i ^ 2) for i in range(4)]
    across_core = [(i, i ^ 1) for i in range(4)]
    inv_freq = ROPE_BASE ** (-np.arange(0, 32, 2, dtype=np.float64) / 32)

    def local_block(hidden, pos_ids, block_ids, ctx_len, ln_gamma, ln_beta, w_qkv, b_qkv, w_dense, b_dense):
        n_rows, blk, width = hidden.shape
        n_heads, _, hd = b_qkv.shape
        heads = n_heads // 2
        rows = heads * hd
        half = rows // 2
        t = lax.axis_index('sp').astype(jnp.int32)
        core = t & 1
        idx = jnp.stack([t, t ^ 1, t ^ 2, t ^ 3, t >> 1, core, 2 + core, 1 - core, 3 - core])
        starts = np.concatenate([[0], np.cumsum(CHUNKS)]).tolist()

        def norm(chunks):
            first = starts[chunks[0]]
            step_rows = 2 if first % 2 == 0 and all(CHUNKS[i] % 2 == 0 for i in chunks) else 1
            plan, specs, shapes = [], [], []
            for i in chunks:
                r0, r1 = starts[i] - first, starts[i + 1] - first
                lo, hi = r0 // step_rows, (r1 - 1) // step_rows
                n = min(step_rows, r1 - r0)
                plan.append((lo, hi, [(r0 + k) % step_rows for k in range(n)]))
                specs.append(pl.BlockSpec((n, width, blk), lambda b, lo=lo, hi=hi: (jnp.clip(b - lo, 0, hi - lo), 0, 0)))
                shapes.append(jax.ShapeDtypeStruct((r1 - r0, width, blk), BF16))
            total = starts[chunks[-1] + 1] - first
            return list(pl.pallas_call(
                functools.partial(norm_kernel, plan),
                grid=(total // step_rows,),
                in_specs=[pl.BlockSpec((step_rows, blk, width), lambda b: (first // step_rows + b, 0, 0)),
                          pl.BlockSpec((width,), lambda b: (0,)),
                          pl.BlockSpec((width,), lambda b: (0,))],
                out_specs=specs,
                out_shape=shapes,
                compiler_params=params(60),
                cost_estimate=pl.CostEstimate(flops=total * 500_000_000, bytes_accessed=total * 800_000, transcendentals=0),
                name="norm",
            )(hidden, ln_gamma, ln_beta))

        a_own = norm([0])
        a_own += norm(list(range(1, len(CHUNKS))))
        a_x = []
        for a in a_own:
            a_x.append(lax.ppermute(a, 'sp', across_x))

        last = pos_ids[:, blk - 1:].reshape(1, n_rows)
        last_x = lax.ppermute(last, 'sp', across_x)
        last_c = lax.ppermute(last, 'sp', across_core)
        last_xc = lax.ppermute(last_x, 'sp', across_core)
        mask_pos = jnp.where(t == 3, last, jnp.where(t == 2, last_c, jnp.where(t == 1, last_x, last_xc)))[0]
        freq = jnp.asarray(inv_freq.astype(np.float32))
        angle = jnp.stack([mask_pos, ctx_len - 1], axis=1).astype(F32)[:, :, None] * freq
        col = jnp.stack([jnp.cos(angle), jnp.sin(angle)], axis=2).reshape(n_rows, 64, 1)
        col = jnp.broadcast_to(col, (n_rows, 64, 128))
        angle = inv_freq[None, :, None] * np.arange(4 * blk).reshape(4, 1, blk)
        tab = jnp.asarray(np.concatenate([np.cos(angle), np.sin(angle)], axis=1).astype(np.float32))

        w = w_qkv.transpose(2, 1, 3, 0).reshape(3, 2, 2, half, width)
        w = lax.dynamic_index_in_dim(w, core, 2, keepdims=False).reshape(3 * rows, width)
        bias = b_qkv.transpose(1, 0, 2).reshape(3, 2, 2, half)
        bias = lax.dynamic_index_in_dim(bias, core, 2, keepdims=False).reshape(3 * rows, 1)
        bias = jnp.broadcast_to(bias.astype(F32), (3 * rows, 128))
        wd = w_dense.reshape(4, half, width)

        keys = values = out = None

        def finish(item, out):
            i, own, other = item
            n, r0 = CHUNKS[i], starts[i]
            extra = [] if out is None else [out]
            return pl.pallas_call(
                dense_kernel,
                grid_spec=pltpu.PrefetchScalarGridSpec(
                    num_scalar_prefetch=1,
                    grid=(n,),
                    in_specs=[pl.BlockSpec((1, blk, rows), lambda b, s: (b, 0, 0)),
                              pl.BlockSpec((1, blk, rows), lambda b, s: (b, 0, 0)),
                              pl.BlockSpec((1, width, blk), lambda b, s: (b, 0, 0))]
                    + [pl.BlockSpec((1, half, width), lambda b, s, k=k: (s[k], 0, 0)) for k in (5, 6, 7, 8)]
                    + [pl.BlockSpec((width,), lambda b, s: (0,))]
                    + [pl.BlockSpec(memory_space=pl.ANY)] * len(extra),
                    out_specs=pl.BlockSpec((1, blk, width), lambda b, s: (r0 + b, 0, 0)),
                ),
                out_shape=jax.ShapeDtypeStruct((n_rows, blk, width), BF16),
                input_output_aliases={9: 0} if extra else {},
                compiler_params=params(24),
                cost_estimate=pl.CostEstimate(flops=n * 1_000_000_000, bytes_accessed=n * 2_000_000, transcendentals=0),
                name="dense",
            )(idx, own, other, a_own[i], wd, wd, wd, wd, b_dense, *extra)

        a_c, a_xc = {}, {}

        def fetch(i, after):
            got = lax.optimization_barrier((a_own[i], a_x[i], *after))
            a_c[i] = lax.ppermute(got[0], 'sp', across_core)
            a_xc[i] = lax.ppermute(got[1], 'sp', across_core)

        fetch(0, (a_own[1], w, bias, col))
        pending = []
        for i, n in enumerate(CHUNKS):
            r0 = starts[i]
            extra = [] if keys is None else [keys, values]
            a_spec = pl.BlockSpec((1, width, blk), lambda b, *_: (b, 0, 0))
            kv_shape = jax.ShapeDtypeStruct((n_rows, half, 4 * blk), BF16)
            kv_spec = pl.BlockSpec((1, half, 4 * blk), lambda b, *_, r0=r0: (r0 + b, 0, 0))
            c_shape = jax.ShapeDtypeStruct((n, blk, rows), BF16)
            c_spec = pl.BlockSpec((1, blk, rows), lambda b, *_: (b, 0, 0))
            attn = pl.pallas_call(
                functools.partial(attn_kernel, heads, r0),
                grid_spec=pltpu.PrefetchScalarGridSpec(
                    num_scalar_prefetch=2,
                    grid=(n,),
                    in_specs=[a_spec] * 4 + [
                        pl.BlockSpec((4, 32, blk), lambda b, *_: (0, 0, 0)),
                        pl.BlockSpec((1, 64, 128), lambda b, *_, r0=r0: (r0 + b, 0, 0)),
                        pl.BlockSpec((3 * rows, width), lambda b, *_: (0, 0)),
                        pl.BlockSpec((3 * rows, 128), lambda b, *_: (0, 0))]
                    + [pl.BlockSpec(memory_space=pl.ANY)] * len(extra),
                    out_specs=[kv_spec, kv_spec, c_spec, c_spec],
                    scratch_shapes=[
                        pltpu.VMEM((4, heads // 2, blk, 128), BF16),
                        pltpu.VMEM((4, rows, blk), BF16),
                        pltpu.VMEM((4, rows, blk), BF16),
                        pltpu.VMEM((2, heads, 128, blk), BF16),
                        pltpu.VMEM((2, 4 * blk, blk), F32),
                        pltpu.VMEM((2, 4 * blk, blk), BF16),
                        pltpu.VMEM((2, rows, blk), BF16),
                        pltpu.VMEM((2, blk, blk), F32),
                    ],
                ),
                out_shape=[kv_shape, kv_shape, c_shape, c_shape],
                input_output_aliases={10: 0, 11: 1} if extra else {},
                compiler_params=params(28),
                cost_estimate=pl.CostEstimate(flops=n * 6_000_000_000, bytes_accessed=n * 4_000_000, transcendentals=0),
                name="attn",
            )
            keys, values, own, send = attn(idx, ctx_len, a_own[i], a_c[i], a_x[i], a_xc[i], tab, col, w, bias, *extra)
            other = lax.ppermute(send, 'sp', across_core)
            if i + 1 < len(CHUNKS):
                fetch(i + 1, (own,) + (() if out is None else (out,)))
            for item in pending:
                out = finish(item, out)
            pending = [(i, own, other)]
        for item in pending:
            out = finish(item, out)

        def by_heads(x):
            return x.reshape(n_rows, n_heads // 4, hd, 4 * blk).transpose(0, 3, 1, 2)

        return out, by_heads(keys), by_heads(values)

    return jax.shard_map(local_block, mesh=mesh, in_specs=(seq_spec, row_spec, row_spec, P('dp'), replicated, replicated, replicated, replicated, replicated, replicated), out_specs=(seq_spec, head_spec, head_spec), check_vma=False)
```

```python
import functools
import math
import numpy as np
import jax
import jax.numpy as jnp
from jax import lax
from jax.experimental import pallas as pl
from jax.experimental.pallas import tpu as pltpu
from jax.sharding import PartitionSpec as P

ALPHA = math.sqrt(56.0)
ROPE_BASE = 10000.0
LN_EPS = 1e-5
LOG2E = 1.4426950408889634
CHUNKS = (4, 3, 3, 3, 3)
F32 = jnp.float32
BF16 = jnp.bfloat16


def mm(a, b):
    return jnp.dot(a, b, preferred_element_type=F32)


def row_vector(ref):
    return ref[...].astype(F32).reshape(1, ref.shape[0])


def norm_kernel(plan, h_ref, g_ref, b_ref, *o_refs):
    def row(r):
        x = h_ref[r].astype(F32)
        x = x - jnp.mean(x, axis=-1, keepdims=True)
        var = jnp.mean(x * x, axis=-1, keepdims=True)
        y = x * lax.rsqrt(var + LN_EPS) * row_vector(g_ref) + row_vector(b_ref)
        return y.astype(BF16).T

    out = [row(r) for r in range(h_ref.shape[0])]
    step = pl.program_id(0)
    for (lo, hi, rows), o_ref in zip(plan, o_refs):
        @pl.when((step >= lo) & (step <= hi))
        def _():
            for i, r in enumerate(rows):
                o_ref[i] = out[r]


def rotate(x, cos_a, sin_a, cos_b, sin_b):
    u0, w0, u1, w1 = (x[16 * i:16 * i + 16] for i in range(4))
    parts = [u0 * cos_a - w0 * sin_a, w0 * cos_a + u0 * sin_a,
             u1 * cos_b - w1 * sin_b, w1 * cos_b + u1 * sin_b]
    return jnp.concatenate(parts, axis=0).astype(BF16)


def fold(accs, x, op):
    accs = list(accs) if accs else [None] * 4
    for i in range(x.shape[0] // 8):
        v = x[8 * i:8 * i + 8]
        accs[i % 4] = v if accs[i % 4] is None else op(accs[i % 4], v)
    return accs


def join(accs, op):
    return op(op(accs[0], accs[1]), op(accs[2], accs[3]))


def attn_kernel(heads, idx_ref, ctx_ref, row_ref, a0, a1, a2, a3, tab_ref, col_ref, w_ref, bias_ref, *rest):
    k_out, v_out, c_own, c_send, kn, kt, vt, qt, s_s, p_s, c_s, m_s = rest[-12:]
    hd = 64
    rows = heads * hd
    blk = a0.shape[2]
    ctx = ctx_ref[row_ref[0] + pl.program_id(0)]

    col = [jnp.concatenate([col_ref[0, 16 * i:16 * i + 16]] * 2, axis=1) for i in range(4)]
    for m, a_ref in enumerate((a0, a1, a2, a3)):
        j = idx_ref[m]
        a = a_ref[0]
        cos, sin = tab_ref[j, :16], tab_ref[j, 16:]
        inside = j * blk + lax.broadcasted_iota(jnp.int32, (1, blk), 1) < ctx
        tab = (jnp.where(inside, cos, col[0]), jnp.where(inside, sin, col[1]),
               jnp.where(inside, 1.0, cos * col[2] + sin * col[3]),
               jnp.where(inside, 0.0, sin * col[2] - cos * col[3]))

        def project(part):
            lo = part * rows
            b = bias_ref[lo:lo + rows]
            return (mm(w_ref[lo:lo + rows], a) + jnp.concatenate([b, b], axis=1)).astype(BF16)

        if m < 2:
            q = project(0)
            for h in range(heads):
                qh = rotate(q[h * hd:(h + 1) * hd].astype(F32), *tab)
                zero = jnp.zeros_like(qh)
                qt[m, h] = jnp.concatenate([qh, zero] if h % 2 == 0 else [zero, qh], axis=0)
        k = project(1)
        for p in range(heads // 2):
            pair = [rotate(k[(2 * p + i) * hd:(2 * p + i + 1) * hd].astype(F32), *tab) for i in range(2)]
            pair = jnp.concatenate(pair, axis=0)
            kt[j, p * 128:(p + 1) * 128] = pair
            kn[j, p] = pair.T
        vt[j] = project(2)

    half = rows // 2
    out_lo = pl.multiple_of(idx_ref[4] * half, half)
    for j in range(4):
        k_out[0, :, j * blk:(j + 1) * blk] = kt[j, pl.ds(out_lo, half)]
        v_out[0, :, j * blk:(j + 1) * blk] = vt[j, pl.ds(out_lo, half)]

    scale = LOG2E / math.sqrt(hd)

    def attend(nb, masked, qi, jq):
        q_pos = jq * blk + lax.broadcasted_iota(jnp.int32, (1, blk), 1)
        limit = jnp.maximum(q_pos, ctx - 1)
        for kb in masked:
            key_pos = kb * blk + lax.broadcasted_iota(jnp.int32, (blk, blk), 0)
            m_s[kb % 2] = jnp.where(key_pos <= limit, 0.0, -jnp.inf)
        top, total, acc = {}, {}, {}
        for step in range(heads + 2):
            h0, h1, h2 = step, step - 1, step - 2
            if 0 <= h1 < heads:
                top[h1] = jnp.max(join(top[h1], jnp.maximum), axis=0, keepdims=True)
            for kb in range(nb):
                lo = kb * blk
                if h0 < heads:
                    s = mm(kn[kb, h0 // 2], qt[qi, h0])
                    if kb in masked:
                        s = s + m_s[kb % 2]
                    s_s[h0 % 2, lo:lo + blk] = s
                    top[h0] = fold(top.get(h0), s, jnp.maximum)
                if 0 <= h1 < heads:
                    for r in range(lo, lo + blk, 32):
                        e = jnp.exp2((s_s[h1 % 2, r:r + 32] - top[h1]) * scale)
                        total[h1] = fold(total.get(h1), e, jnp.add)
                        p_s[h1 % 2, r:r + 32] = e.astype(BF16)
                if 0 <= h2 < heads:
                    t = mm(vt[kb, h2 * hd:(h2 + 1) * hd], p_s[h2 % 2, lo:lo + blk])
                    acc[h2] = acc[h2] + t if kb else t
            if 0 <= h2 < heads:
                t = jnp.sum(join(total[h2], jnp.add), axis=0, keepdims=True)
                c_s[qi, h2 * hd:(h2 + 1) * hd] = (acc[h2] / t).astype(BF16)

    def query_block(qi, carry):
        jq = idx_ref[qi]
        pl.when(jq < 3)(functools.partial(attend, 3, (1, 2), qi, jq))
        pl.when(jq == 3)(functools.partial(attend, 4, (3,), qi, jq))
        return carry

    lax.fori_loop(0, 2, query_block, 0)
    c_own[0] = c_s[0].T
    c_send[0] = c_s[1].T


def dense_kernel(idx_ref, row_ref, own_ref, other_ref, a_ref, w0, w1, w2, w3, b_ref, *rest):
    o_ref = rest[-1]
    for r in range(o_ref.shape[0]):
        w = jnp.concatenate([w0[0], w1[0]], axis=0)
        acc = mm(own_ref[r], w)
        w = jnp.concatenate([w2[0], w3[0]], axis=0)
        acc = acc + mm(other_ref[r], w)
        o_ref[r] = (a_ref[r].T.astype(F32) * ALPHA + (acc + row_vector(b_ref))).astype(BF16)


def params(mib):
    return pltpu.CompilerParams(dimension_semantics=("arbitrary",), vmem_limit_bytes=mib * 1024 * 1024)


def solution(mesh):
    seq_spec = P('dp', 'sp', None)
    row_spec = P('dp', 'sp')
    head_spec = P('dp', None, 'sp', None)
    replicated = P()
    across_x = [(i, i ^ 2) for i in range(4)]
    across_core = [(i, i ^ 1) for i in range(4)]
    inv_freq = ROPE_BASE ** (-np.arange(0, 32, 2, dtype=np.float64) / 32)

    def local_block(hidden, pos_ids, block_ids, ctx_len, ln_gamma, ln_beta, w_qkv, b_qkv, w_dense, b_dense):
        n_rows, blk, width = hidden.shape
        n_heads, _, hd = b_qkv.shape
        heads = n_heads // 2
        rows = heads * hd
        half = rows // 2
        t = lax.axis_index('sp').astype(jnp.int32)
        core = t & 1
        idx = jnp.stack([t, t ^ 1, t ^ 2, t ^ 3, t >> 1, core, 2 + core, 1 - core, 3 - core])
        starts = np.concatenate([[0], np.cumsum(CHUNKS)]).tolist()

        def norm(chunks):
            first = starts[chunks[0]]
            step_rows = 2 if first % 2 == 0 and all(CHUNKS[i] % 2 == 0 for i in chunks) else 1
            plan, specs, shapes = [], [], []
            for i in chunks:
                r0, r1 = starts[i] - first, starts[i + 1] - first
                lo, hi = r0 // step_rows, (r1 - 1) // step_rows
                n = min(step_rows, r1 - r0)
                plan.append((lo, hi, [(r0 + k) % step_rows for k in range(n)]))
                specs.append(pl.BlockSpec((n, width, blk), lambda b, lo=lo, hi=hi: (jnp.clip(b - lo, 0, hi - lo), 0, 0)))
                shapes.append(jax.ShapeDtypeStruct((r1 - r0, width, blk), BF16))
            total = starts[chunks[-1] + 1] - first
            return list(pl.pallas_call(
                functools.partial(norm_kernel, plan),
                grid=(total // step_rows,),
                in_specs=[pl.BlockSpec((step_rows, blk, width), lambda b: (first // step_rows + b, 0, 0)),
                          pl.BlockSpec((width,), lambda b: (0,)),
                          pl.BlockSpec((width,), lambda b: (0,))],
                out_specs=specs,
                out_shape=shapes,
                compiler_params=params(60),
                cost_estimate=pl.CostEstimate(flops=total * 500_000_000, bytes_accessed=total * 800_000, transcendentals=0),
                name="norm",
            )(hidden, ln_gamma, ln_beta))

        a_own = norm([0])
        a_own += norm(list(range(1, len(CHUNKS))))
        a_x = []
        for a in a_own:
            a_x.append(lax.ppermute(a, 'sp', across_x))
        a_c = []
        for a in a_own:
            a_c.append(lax.ppermute(a, 'sp', across_core))

        last = pos_ids[:, blk - 1:].reshape(1, n_rows)
        last_x = lax.ppermute(last, 'sp', across_x)
        last_c = lax.ppermute(last, 'sp', across_core)
        last_xc = lax.ppermute(last_x, 'sp', across_core)
        mask_pos = jnp.where(t == 3, last, jnp.where(t == 2, last_c, jnp.where(t == 1, last_x, last_xc)))[0]
        freq = jnp.asarray(inv_freq.astype(np.float32))
        angle = jnp.stack([mask_pos, ctx_len - 1], axis=1).astype(F32)[:, :, None] * freq
        col = jnp.stack([jnp.cos(angle), jnp.sin(angle)], axis=2).reshape(n_rows, 64, 1)
        col = jnp.broadcast_to(col, (n_rows, 64, 128))
        angle = inv_freq[None, :, None] * np.arange(4 * blk).reshape(4, 1, blk)
        tab = jnp.asarray(np.concatenate([np.cos(angle), np.sin(angle)], axis=1).astype(np.float32))

        w = w_qkv.transpose(2, 1, 3, 0).reshape(3, 2, 2, half, width)
        w = lax.dynamic_index_in_dim(w, core, 2, keepdims=False).reshape(3 * rows, width)
        bias = b_qkv.transpose(1, 0, 2).reshape(3, 2, 2, half)
        bias = lax.dynamic_index_in_dim(bias, core, 2, keepdims=False).reshape(3 * rows, 1)
        bias = jnp.broadcast_to(bias.astype(F32), (3 * rows, 128))
        wd = w_dense.reshape(4, half, width)

        row_of = [jnp.full((1,), r, jnp.int32) for r in starts[:-1]]

        keys = values = out = None

        def finish(item, out):
            i, own, other = item
            n = CHUNKS[i]
            extra = [] if out is None else [out]
            return pl.pallas_call(
                dense_kernel,
                grid_spec=pltpu.PrefetchScalarGridSpec(
                    num_scalar_prefetch=2,
                    grid=(n,),
                    in_specs=[pl.BlockSpec((1, blk, rows), lambda b, s, r: (b, 0, 0)),
                              pl.BlockSpec((1, blk, rows), lambda b, s, r: (b, 0, 0)),
                              pl.BlockSpec((1, width, blk), lambda b, s, r: (b, 0, 0))]
                    + [pl.BlockSpec((1, half, width), lambda b, s, r, k=k: (s[k], 0, 0)) for k in (5, 6, 7, 8)]
                    + [pl.BlockSpec((width,), lambda b, s, r: (0,))]
                    + [pl.BlockSpec(memory_space=pl.ANY)] * len(extra),
                    out_specs=pl.BlockSpec((1, blk, width), lambda b, s, r: (r[0] + b, 0, 0)),
                ),
                out_shape=jax.ShapeDtypeStruct((n_rows, blk, width), BF16),
                input_output_aliases={10: 0} if extra else {},
                compiler_params=params(24),
                cost_estimate=pl.CostEstimate(flops=n * 1_000_000_000, bytes_accessed=n * 2_000_000, transcendentals=0),
                name="dense",
            )(idx, row_of[i], own, other, a_own[i], wd, wd, wd, wd, b_dense, *extra)

        a_xc = {}

        def fetch(i, after):
            got = lax.optimization_barrier((a_x[i], *after))
            a_xc[i] = lax.ppermute(got[0], 'sp', across_core)

        fetch(0, (a_own[1], w, bias, col))
        pending = []
        for i, n in enumerate(CHUNKS):
            extra = [] if keys is None else [keys, values]
            a_spec = pl.BlockSpec((1, width, blk), lambda b, *_: (b, 0, 0))
            kv_shape = jax.ShapeDtypeStruct((n_rows, half, 4 * blk), BF16)
            kv_spec = pl.BlockSpec((1, half, 4 * blk), lambda b, i, c, r: (r[0] + b, 0, 0))
            c_shape = jax.ShapeDtypeStruct((n, blk, rows), BF16)
            c_spec = pl.BlockSpec((1, blk, rows), lambda b, *_: (b, 0, 0))
            attn = pl.pallas_call(
                functools.partial(attn_kernel, heads),
                grid_spec=pltpu.PrefetchScalarGridSpec(
                    num_scalar_prefetch=3,
                    grid=(n,),
                    in_specs=[a_spec] * 4 + [
                        pl.BlockSpec((4, 32, blk), lambda b, *_: (0, 0, 0)),
                        pl.BlockSpec((1, 64, 128), lambda b, i, c, r: (r[0] + b, 0, 0)),
                        pl.BlockSpec((3 * rows, width), lambda b, *_: (0, 0)),
                        pl.BlockSpec((3 * rows, 128), lambda b, *_: (0, 0))]
                    + [pl.BlockSpec(memory_space=pl.ANY)] * len(extra),
                    out_specs=[kv_spec, kv_spec, c_spec, c_spec],
                    scratch_shapes=[
                        pltpu.VMEM((4, heads // 2, blk, 128), BF16),
                        pltpu.VMEM((4, rows, blk), BF16),
                        pltpu.VMEM((4, rows, blk), BF16),
                        pltpu.VMEM((2, heads, 128, blk), BF16),
                        pltpu.VMEM((2, 4 * blk, blk), F32),
                        pltpu.VMEM((2, 4 * blk, blk), BF16),
                        pltpu.VMEM((2, rows, blk), BF16),
                        pltpu.VMEM((2, blk, blk), F32),
                    ],
                ),
                out_shape=[kv_shape, kv_shape, c_shape, c_shape],
                input_output_aliases={11: 0, 12: 1} if extra else {},
                compiler_params=params(28),
                cost_estimate=pl.CostEstimate(flops=n * 6_000_000_000, bytes_accessed=n * 4_000_000, transcendentals=0),
                name="attn",
            )
            keys, values, own, send = attn(idx, ctx_len, row_of[i], a_own[i], a_c[i], a_x[i], a_xc[i], tab, col, w, bias, *extra)
            other = lax.ppermute(send, 'sp', across_core)
            if i + 1 < len(CHUNKS):
                fetch(i + 1, (own,) + (() if out is None else (out,)))
            for item in pending:
                out = finish(item, out)
            pending = [(i, own, other)]
        for item in pending:
            out = finish(item, out)

        def by_heads(x):
            return x.reshape(n_rows, n_heads // 4, hd, 4 * blk).transpose(0, 3, 1, 2)

        return out, by_heads(keys), by_heads(values)

    return jax.shard_map(local_block, mesh=mesh, in_specs=(seq_spec, row_spec, row_spec, P('dp'), replicated, replicated, replicated, replicated, replicated, replicated), out_specs=(seq_spec, head_spec, head_spec), check_vma=False)
```

```python
import functools
import math
import numpy as np
import jax
import jax.numpy as jnp
from jax import lax
from jax.experimental import pallas as pl
from jax.experimental.pallas import tpu as pltpu
from jax.sharding import PartitionSpec as P

ALPHA = math.sqrt(56.0)
ROPE_BASE = 10000.0
LN_EPS = 1e-5
LOG2E = 1.4426950408889634
CHUNKS = (1, 3, 3, 3, 3, 3)
F32 = jnp.float32
BF16 = jnp.bfloat16


def mm(a, b):
    return jnp.dot(a, b, preferred_element_type=F32)


def row_vector(ref):
    return ref[...].astype(F32).reshape(1, ref.shape[0])


def norm_kernel(plan, h_ref, g_ref, b_ref, *o_refs):
    def row(r):
        x = h_ref[r].astype(F32)
        x = x - jnp.mean(x, axis=-1, keepdims=True)
        var = jnp.mean(x * x, axis=-1, keepdims=True)
        y = x * lax.rsqrt(var + LN_EPS) * row_vector(g_ref) + row_vector(b_ref)
        return y.astype(BF16).T

    out = [row(r) for r in range(h_ref.shape[0])]
    step = pl.program_id(0)
    for (lo, hi, rows), o_ref in zip(plan, o_refs):
        @pl.when((step >= lo) & (step <= hi))
        def _():
            for i, r in enumerate(rows):
                o_ref[i] = out[r]


def rotate(x, cos_a, sin_a, cos_b, sin_b):
    u0, w0, u1, w1 = (x[16 * i:16 * i + 16] for i in range(4))
    parts = [u0 * cos_a - w0 * sin_a, w0 * cos_a + u0 * sin_a,
             u1 * cos_b - w1 * sin_b, w1 * cos_b + u1 * sin_b]
    return jnp.concatenate(parts, axis=0).astype(BF16)


def fold(accs, x, op):
    accs = list(accs) if accs else [None] * 4
    for i in range(x.shape[0] // 8):
        v = x[8 * i:8 * i + 8]
        accs[i % 4] = v if accs[i % 4] is None else op(accs[i % 4], v)
    return accs


def join(accs, op):
    return op(op(accs[0], accs[1]), op(accs[2], accs[3]))


def attn_kernel(heads, idx_ref, ctx_ref, row_ref, a0, a1, a2, a3, tab_ref, col_ref, w_ref, bias_ref, *rest):
    k_out, v_out, c_own, c_send, kn, kt, vt, qt, s_s, p_s, c_s, m_s = rest[-12:]
    hd = 64
    rows = heads * hd
    blk = a0.shape[2]
    ctx = ctx_ref[row_ref[0] + pl.program_id(0)]

    col = [jnp.concatenate([col_ref[0, 16 * i:16 * i + 16]] * 2, axis=1) for i in range(4)]
    for m, a_ref in enumerate((a0, a1, a2, a3)):
        j = idx_ref[m]
        a = a_ref[0]
        cos, sin = tab_ref[j, :16], tab_ref[j, 16:]
        inside = j * blk + lax.broadcasted_iota(jnp.int32, (1, blk), 1) < ctx
        tab = (jnp.where(inside, cos, col[0]), jnp.where(inside, sin, col[1]),
               jnp.where(inside, 1.0, cos * col[2] + sin * col[3]),
               jnp.where(inside, 0.0, sin * col[2] - cos * col[3]))

        def project(part):
            lo = part * rows
            b = bias_ref[lo:lo + rows]
            return (mm(w_ref[lo:lo + rows], a) + jnp.concatenate([b, b], axis=1)).astype(BF16)

        if m < 2:
            q = project(0)
            for h in range(heads):
                qh = rotate(q[h * hd:(h + 1) * hd].astype(F32), *tab)
                zero = jnp.zeros_like(qh)
                qt[m, h] = jnp.concatenate([qh, zero] if h % 2 == 0 else [zero, qh], axis=0)
        k = project(1)
        for p in range(heads // 2):
            pair = [rotate(k[(2 * p + i) * hd:(2 * p + i + 1) * hd].astype(F32), *tab) for i in range(2)]
            pair = jnp.concatenate(pair, axis=0)
            kt[j, p * 128:(p + 1) * 128] = pair
            kn[j, p] = pair.T
        vt[j] = project(2)

    half = rows // 2
    out_lo = pl.multiple_of(idx_ref[4] * half, half)

    def copy_out(j, carry):
        to = pl.ds(pl.multiple_of(j * blk, blk), blk)
        k_out[0, :, to] = kt[j, pl.ds(out_lo, half)]
        v_out[0, :, to] = vt[j, pl.ds(out_lo, half)]
        return carry

    lax.fori_loop(0, 4, copy_out, 0)

    scale = LOG2E / math.sqrt(hd)

    def attend(nb, masked, qi, jq):
        q_pos = jq * blk + lax.broadcasted_iota(jnp.int32, (1, blk), 1)
        limit = jnp.maximum(q_pos, ctx - 1)
        for kb in masked:
            key_pos = kb * blk + lax.broadcasted_iota(jnp.int32, (blk, blk), 0)
            m_s[kb % 2] = jnp.where(key_pos <= limit, 0.0, -jnp.inf)
        top, total, acc = {}, {}, {}
        for step in range(heads + 2):
            h0, h1, h2 = step, step - 1, step - 2
            if 0 <= h1 < heads:
                top[h1] = jnp.max(join(top[h1], jnp.maximum), axis=0, keepdims=True)
            for kb in range(nb):
                lo = kb * blk
                if h0 < heads:
                    s = mm(kn[kb, h0 // 2], qt[qi, h0])
                    if kb in masked:
                        s = s + m_s[kb % 2]
                    s_s[h0 % 2, lo:lo + blk] = s
                    top[h0] = fold(top.get(h0), s, jnp.maximum)
                if 0 <= h1 < heads:
                    for r in range(lo, lo + blk, 32):
                        e = jnp.exp2((s_s[h1 % 2, r:r + 32] - top[h1]) * scale)
                        total[h1] = fold(total.get(h1), e, jnp.add)
                        p_s[h1 % 2, r:r + 32] = e.astype(BF16)
                if 0 <= h2 < heads:
                    t = mm(vt[kb, h2 * hd:(h2 + 1) * hd], p_s[h2 % 2, lo:lo + blk])
                    acc[h2] = acc[h2] + t if kb else t
            if 0 <= h2 < heads:
                t = jnp.sum(join(total[h2], jnp.add), axis=0, keepdims=True)
                c_s[qi, h2 * hd:(h2 + 1) * hd] = (acc[h2] / t).astype(BF16)

    def query_block(qi, carry):
        jq = idx_ref[qi]
        pl.when(jq < 3)(functools.partial(attend, 3, (1, 2), qi, jq))
        pl.when(jq == 3)(functools.partial(attend, 4, (3,), qi, jq))
        return carry

    lax.fori_loop(0, 2, query_block, 0)
    c_own[0] = c_s[0].T
    c_send[0] = c_s[1].T


def dense_kernel(idx_ref, row_ref, own_ref, other_ref, a_ref, w0, w1, w2, w3, b_ref, *rest):
    o_ref = rest[-1]
    tile = 256

    def columns(t, carry):
        lo = pl.ds(pl.multiple_of(t * tile, tile), tile)
        w = jnp.concatenate([w0[0, :, lo], w1[0, :, lo]], axis=0)
        acc = mm(own_ref[0], w)
        w = jnp.concatenate([w2[0, :, lo], w3[0, :, lo]], axis=0)
        acc = acc + mm(other_ref[0], w)
        o_ref[0, :, lo] = (a_ref[0, lo].T.astype(F32) * ALPHA + (acc + b_ref[:, lo].astype(F32))).astype(BF16)
        return carry

    lax.fori_loop(0, o_ref.shape[2] // tile, columns, 0)


def params(mib):
    return pltpu.CompilerParams(dimension_semantics=("arbitrary",), vmem_limit_bytes=mib * 1024 * 1024)


def solution(mesh):
    seq_spec = P('dp', 'sp', None)
    row_spec = P('dp', 'sp')
    head_spec = P('dp', None, 'sp', None)
    replicated = P()
    across_x = [(i, i ^ 2) for i in range(4)]
    across_core = [(i, i ^ 1) for i in range(4)]
    inv_freq = ROPE_BASE ** (-np.arange(0, 32, 2, dtype=np.float64) / 32)

    def local_block(hidden, pos_ids, block_ids, ctx_len, ln_gamma, ln_beta, w_qkv, b_qkv, w_dense, b_dense):
        n_rows, blk, width = hidden.shape
        n_heads, _, hd = b_qkv.shape
        heads = n_heads // 2
        rows = heads * hd
        half = rows // 2
        t = lax.axis_index('sp').astype(jnp.int32)
        core = t & 1
        idx = jnp.stack([t, t ^ 1, t ^ 2, t ^ 3, t >> 1, core, 2 + core, 1 - core, 3 - core])
        starts = np.concatenate([[0], np.cumsum(CHUNKS)]).tolist()

        def norm(chunks):
            first = starts[chunks[0]]
            step_rows = 2 if first % 2 == 0 and all(CHUNKS[i] % 2 == 0 for i in chunks) else 1
            plan, specs, shapes = [], [], []
            for i in chunks:
                r0, r1 = starts[i] - first, starts[i + 1] - first
                lo, hi = r0 // step_rows, (r1 - 1) // step_rows
                n = min(step_rows, r1 - r0)
                plan.append((lo, hi, [(r0 + k) % step_rows for k in range(n)]))
                specs.append(pl.BlockSpec((n, width, blk), lambda b, lo=lo, hi=hi: (jnp.clip(b - lo, 0, hi - lo), 0, 0)))
                shapes.append(jax.ShapeDtypeStruct((r1 - r0, width, blk), BF16))
            total = starts[chunks[-1] + 1] - first
            return list(pl.pallas_call(
                functools.partial(norm_kernel, plan),
                grid=(total // step_rows,),
                in_specs=[pl.BlockSpec((step_rows, blk, width), lambda b: (first // step_rows + b, 0, 0)),
                          pl.BlockSpec((width,), lambda b: (0,)),
                          pl.BlockSpec((width,), lambda b: (0,))],
                out_specs=specs,
                out_shape=shapes,
                compiler_params=params(60),
                cost_estimate=pl.CostEstimate(flops=total * 500_000_000, bytes_accessed=total * 800_000, transcendentals=0),
                name="norm",
            )(hidden, ln_gamma, ln_beta))

        a_own = norm([0])
        a_own += norm(list(range(1, len(CHUNKS))))
        a_x = []
        for a in a_own:
            a_x.append(lax.ppermute(a, 'sp', across_x))
        a_c = []
        for a in a_own:
            a_c.append(lax.ppermute(a, 'sp', across_core))

        last = pos_ids[:, blk - 1:].reshape(1, n_rows)
        last_x = lax.ppermute(last, 'sp', across_x)
        last_c = lax.ppermute(last, 'sp', across_core)
        last_xc = lax.ppermute(last_x, 'sp', across_core)
        mask_pos = jnp.where(t == 3, last, jnp.where(t == 2, last_c, jnp.where(t == 1, last_x, last_xc)))[0]
        freq = jnp.asarray(inv_freq.astype(np.float32))
        angle = jnp.stack([mask_pos, ctx_len - 1], axis=1).astype(F32)[:, :, None] * freq
        col = jnp.stack([jnp.cos(angle), jnp.sin(angle)], axis=2).reshape(n_rows, 64, 1)
        col = jnp.broadcast_to(col, (n_rows, 64, 128))
        fine = inv_freq[:, None] * np.arange(blk)
        fine_c, fine_s = np.cos(fine).astype(np.float32)[None], np.sin(fine).astype(np.float32)[None]
        coarse = inv_freq[None, :, None] * (np.arange(4) * blk)[:, None, None]
        coarse_c, coarse_s = np.cos(coarse).astype(np.float32), np.sin(coarse).astype(np.float32)
        tab = jnp.concatenate([fine_c * jnp.asarray(coarse_c) - fine_s * jnp.asarray(coarse_s),
                               fine_s * jnp.asarray(coarse_c) + fine_c * jnp.asarray(coarse_s)], axis=1)

        bias = b_qkv.transpose(1, 0, 2).reshape(3, 2, 2, half)
        bias = lax.dynamic_index_in_dim(bias, core, 2, keepdims=False).reshape(3 * rows, 1)
        bias = jnp.broadcast_to(bias.astype(F32), (3 * rows, 128))
        w, bias, col, tab = lax.optimization_barrier((w_qkv, bias, col, tab))
        w = w.transpose(2, 1, 3, 0).reshape(3, 2, 2, half, width)
        w = lax.dynamic_index_in_dim(w, core, 2, keepdims=False).reshape(3 * rows, width)
        wd = w_dense.reshape(4, half, width)

        row_of = [jnp.full((1,), r, jnp.int32) for r in starts[:-1]]

        keys = values = out = None

        def finish(item, out):
            i, own, other = item
            n = CHUNKS[i]
            extra = [] if out is None else [out]
            return pl.pallas_call(
                dense_kernel,
                grid_spec=pltpu.PrefetchScalarGridSpec(
                    num_scalar_prefetch=2,
                    grid=(n,),
                    in_specs=[pl.BlockSpec((1, blk, rows), lambda b, s, r: (b, 0, 0)),
                              pl.BlockSpec((1, blk, rows), lambda b, s, r: (b, 0, 0)),
                              pl.BlockSpec((1, width, blk), lambda b, s, r: (b, 0, 0))]
                    + [pl.BlockSpec((1, half, width), lambda b, s, r, k=k: (s[k], 0, 0)) for k in (5, 6, 7, 8)]
                    + [pl.BlockSpec((1, width), lambda b, s, r: (0, 0))]
                    + [pl.BlockSpec(memory_space=pl.ANY)] * len(extra),
                    out_specs=pl.BlockSpec((1, blk, width), lambda b, s, r: (r[0] + b, 0, 0)),
                ),
                out_shape=jax.ShapeDtypeStruct((n_rows, blk, width), BF16),
                input_output_aliases={10: 0} if extra else {},
                compiler_params=params(24),
                cost_estimate=pl.CostEstimate(flops=n * 1_000_000_000, bytes_accessed=n * 2_000_000, transcendentals=0),
                name="dense",
            )(idx, row_of[i], own, other, a_own[i], wd, wd, wd, wd, b_dense.reshape(1, width), *extra)

        a_xc = {}

        def fetch(i, after):
            got = lax.optimization_barrier((a_x[i], *after))
            a_xc[i] = lax.ppermute(got[0], 'sp', across_core)

        fetch(0, (a_own[1], w, bias, col))
        pending = []
        for i, n in enumerate(CHUNKS):
            extra = [] if keys is None else [keys, values]
            a_spec = pl.BlockSpec((1, width, blk), lambda b, *_: (b, 0, 0))
            kv_shape = jax.ShapeDtypeStruct((n_rows, half, 4 * blk), BF16)
            kv_spec = pl.BlockSpec((1, half, 4 * blk), lambda b, i, c, r: (r[0] + b, 0, 0))
            c_shape = jax.ShapeDtypeStruct((n, blk, rows), BF16)
            c_spec = pl.BlockSpec((1, blk, rows), lambda b, *_: (b, 0, 0))
            attn = pl.pallas_call(
                functools.partial(attn_kernel, heads),
                grid_spec=pltpu.PrefetchScalarGridSpec(
                    num_scalar_prefetch=3,
                    grid=(n,),
                    in_specs=[a_spec] * 4 + [
                        pl.BlockSpec((4, 32, blk), lambda b, *_: (0, 0, 0)),
                        pl.BlockSpec((1, 64, 128), lambda b, i, c, r: (r[0] + b, 0, 0)),
                        pl.BlockSpec((3 * rows, width), lambda b, *_: (0, 0)),
                        pl.BlockSpec((3 * rows, 128), lambda b, *_: (0, 0))]
                    + [pl.BlockSpec(memory_space=pl.ANY)] * len(extra),
                    out_specs=[kv_spec, kv_spec, c_spec, c_spec],
                    scratch_shapes=[
                        pltpu.VMEM((4, heads // 2, blk, 128), BF16),
                        pltpu.VMEM((4, rows, blk), BF16),
                        pltpu.VMEM((4, rows, blk), BF16),
                        pltpu.VMEM((2, heads, 128, blk), BF16),
                        pltpu.VMEM((2, 4 * blk, blk), F32),
                        pltpu.VMEM((2, 4 * blk, blk), BF16),
                        pltpu.VMEM((2, rows, blk), BF16),
                        pltpu.VMEM((2, blk, blk), F32),
                    ],
                ),
                out_shape=[kv_shape, kv_shape, c_shape, c_shape],
                input_output_aliases={11: 0, 12: 1} if extra else {},
                compiler_params=params(28),
                cost_estimate=pl.CostEstimate(flops=n * 6_000_000_000, bytes_accessed=n * 4_000_000, transcendentals=0),
                name="attn",
            )
            keys, values, own, send = attn(idx, ctx_len, row_of[i], a_own[i], a_c[i], a_x[i], a_xc[i], tab, col, w, bias, *extra)
            other = lax.ppermute(send, 'sp', across_core)
            if i + 1 < len(CHUNKS):
                fetch(i + 1, (own,) + (() if out is None else (out,)))
            for item in pending:
                out = finish(item, out)
            pending = [(i, own, other)]
        for item in pending:
            out = finish(item, out)

        def by_heads(x):
            return x.reshape(n_rows, n_heads // 4, hd, 4 * blk).transpose(0, 3, 1, 2)

        return out, by_heads(keys), by_heads(values)

    return jax.shard_map(local_block, mesh=mesh, in_specs=(seq_spec, row_spec, row_spec, P('dp'), replicated, replicated, replicated, replicated, replicated, replicated), out_specs=(seq_spec, head_spec, head_spec), check_vma=False)
```

```python
import functools
import math
import numpy as np
import jax
import jax.numpy as jnp
from jax import lax
from jax.experimental import pallas as pl
from jax.experimental.pallas import tpu as pltpu
from jax.sharding import PartitionSpec as P

ALPHA = math.sqrt(56.0)
ROPE_BASE = 10000.0
LN_EPS = 1e-5
LOG2E = 1.4426950408889634
CHUNKS = (3, 4, 3, 3, 3)
F32 = jnp.float32
BF16 = jnp.bfloat16


def mm(a, b):
    return jnp.dot(a, b, preferred_element_type=F32)


def row_vector(ref):
    return ref[...].astype(F32).reshape(1, ref.shape[0])


def norm_kernel(plan, h_ref, g_ref, b_ref, *o_refs):
    def row(r):
        x = h_ref[r].astype(F32)
        x = x - jnp.mean(x, axis=-1, keepdims=True)
        var = jnp.mean(x * x, axis=-1, keepdims=True)
        y = x * lax.rsqrt(var + LN_EPS) * row_vector(g_ref) + row_vector(b_ref)
        return y.astype(BF16).T

    out = [row(r) for r in range(h_ref.shape[0])]
    step = pl.program_id(0)
    for (lo, hi, rows), o_ref in zip(plan, o_refs):
        @pl.when((step >= lo) & (step <= hi))
        def _():
            for i, r in enumerate(rows):
                o_ref[i] = out[r]


def rotate(x, cos_a, sin_a, cos_b, sin_b):
    u0, w0, u1, w1 = (x[16 * i:16 * i + 16] for i in range(4))
    parts = [u0 * cos_a - w0 * sin_a, w0 * cos_a + u0 * sin_a,
             u1 * cos_b - w1 * sin_b, w1 * cos_b + u1 * sin_b]
    return jnp.concatenate(parts, axis=0).astype(BF16)


def fold(accs, x, op):
    accs = list(accs) if accs else [None] * 4
    for i in range(x.shape[0] // 8):
        v = x[8 * i:8 * i + 8]
        accs[i % 4] = v if accs[i % 4] is None else op(accs[i % 4], v)
    return accs


def join(accs, op):
    return op(op(accs[0], accs[1]), op(accs[2], accs[3]))


def attn_kernel(heads, idx_ref, ctx_ref, row_ref, a0, a1, a2, a3, tab_ref, col_ref, w_ref, bias_ref, *rest):
    k_out, v_out, c_own, c_send, kn, kt, vt, qt, s_s, p_s, c_s, m_s = rest[-12:]
    hd = 64
    rows = heads * hd
    blk = a0.shape[2]
    ctx = ctx_ref[row_ref[0] + pl.program_id(0)]

    col = [jnp.concatenate([col_ref[0, 16 * i:16 * i + 16]] * 2, axis=1) for i in range(4)]
    for m, a_ref in enumerate((a0, a1, a2, a3)):
        j = idx_ref[m]
        a = a_ref[0]
        cos, sin = tab_ref[j, :16], tab_ref[j, 16:]
        inside = j * blk + lax.broadcasted_iota(jnp.int32, (1, blk), 1) < ctx
        tab = (jnp.where(inside, cos, col[0]), jnp.where(inside, sin, col[1]),
               jnp.where(inside, 1.0, cos * col[2] + sin * col[3]),
               jnp.where(inside, 0.0, sin * col[2] - cos * col[3]))

        def project(part):
            lo = part * rows
            b = bias_ref[lo:lo + rows]
            return (mm(w_ref[lo:lo + rows], a) + jnp.concatenate([b, b], axis=1)).astype(BF16)

        if m < 2:
            q = project(0)
            for h in range(heads):
                qh = rotate(q[h * hd:(h + 1) * hd].astype(F32), *tab)
                zero = jnp.zeros_like(qh)
                qt[m, h] = jnp.concatenate([qh, zero] if h % 2 == 0 else [zero, qh], axis=0)
        k = project(1)
        for p in range(heads // 2):
            pair = [rotate(k[(2 * p + i) * hd:(2 * p + i + 1) * hd].astype(F32), *tab) for i in range(2)]
            pair = jnp.concatenate(pair, axis=0)
            kt[j, p * 128:(p + 1) * 128] = pair
            kn[j, p] = pair.T
        vt[j] = project(2)

    half = rows // 2
    out_lo = pl.multiple_of(idx_ref[4] * half, half)

    def copy_out(j, carry):
        to = pl.ds(pl.multiple_of(j * blk, blk), blk)
        k_out[0, :, to] = kt[j, pl.ds(out_lo, half)]
        v_out[0, :, to] = vt[j, pl.ds(out_lo, half)]
        return carry

    lax.fori_loop(0, 4, copy_out, 0)

    scale = LOG2E / math.sqrt(hd)

    def attend(nb, masked, qi, jq):
        q_pos = jq * blk + lax.broadcasted_iota(jnp.int32, (1, blk), 1)
        limit = jnp.maximum(q_pos, ctx - 1)
        for kb in masked:
            key_pos = kb * blk + lax.broadcasted_iota(jnp.int32, (blk, blk), 0)
            m_s[kb % 2] = jnp.where(key_pos <= limit, 0.0, -jnp.inf)
        top, total, acc = {}, {}, {}
        for step in range(heads + 2):
            h0, h1, h2 = step, step - 1, step - 2
            if 0 <= h1 < heads:
                top[h1] = jnp.max(join(top[h1], jnp.maximum), axis=0, keepdims=True)
            for kb in range(nb):
                lo = kb * blk
                if h0 < heads:
                    s = mm(kn[kb, h0 // 2], qt[qi, h0])
                    if kb in masked:
                        s = s + m_s[kb % 2]
                    s_s[h0 % 2, lo:lo + blk] = s
                    top[h0] = fold(top.get(h0), s, jnp.maximum)
                if 0 <= h1 < heads:
                    for r in range(lo, lo + blk, 32):
                        e = jnp.exp2((s_s[h1 % 2, r:r + 32] - top[h1]) * scale)
                        total[h1] = fold(total.get(h1), e, jnp.add)
                        p_s[h1 % 2, r:r + 32] = e.astype(BF16)
                if 0 <= h2 < heads:
                    t = mm(vt[kb, h2 * hd:(h2 + 1) * hd], p_s[h2 % 2, lo:lo + blk])
                    acc[h2] = acc[h2] + t if kb else t
            if 0 <= h2 < heads:
                t = jnp.sum(join(total[h2], jnp.add), axis=0, keepdims=True)
                c_s[qi, h2 * hd:(h2 + 1) * hd] = (acc[h2] / t).astype(BF16)

    def query_block(qi, carry):
        jq = idx_ref[qi]
        pl.when(jq < 3)(functools.partial(attend, 3, (1, 2), qi, jq))
        pl.when(jq == 3)(functools.partial(attend, 4, (3,), qi, jq))
        return carry

    lax.fori_loop(0, 2, query_block, 0)
    c_own[0] = c_s[0].T
    c_send[0] = c_s[1].T


def dense_kernel(idx_ref, row_ref, own_ref, other_ref, a_ref, w0, w1, w2, w3, b_ref, *rest):
    o_ref = rest[-1]
    for r in range(o_ref.shape[0]):
        w = jnp.concatenate([w0[0], w1[0]], axis=0)
        acc = mm(own_ref[r], w)
        w = jnp.concatenate([w2[0], w3[0]], axis=0)
        acc = acc + mm(other_ref[r], w)
        o_ref[r] = (a_ref[r].T.astype(F32) * ALPHA + (acc + row_vector(b_ref))).astype(BF16)


def params(mib):
    return pltpu.CompilerParams(dimension_semantics=("arbitrary",), vmem_limit_bytes=mib * 1024 * 1024)


def solution(mesh):
    seq_spec = P('dp', 'sp', None)
    row_spec = P('dp', 'sp')
    head_spec = P('dp', None, 'sp', None)
    replicated = P()
    across_x = [(i, i ^ 2) for i in range(4)]
    across_core = [(i, i ^ 1) for i in range(4)]
    inv_freq = ROPE_BASE ** (-np.arange(0, 32, 2, dtype=np.float64) / 32)

    def local_block(hidden, pos_ids, block_ids, ctx_len, ln_gamma, ln_beta, w_qkv, b_qkv, w_dense, b_dense):
        n_rows, blk, width = hidden.shape
        n_heads, _, hd = b_qkv.shape
        heads = n_heads // 2
        rows = heads * hd
        half = rows // 2
        t = lax.axis_index('sp').astype(jnp.int32)
        core = t & 1
        idx = jnp.stack([t, t ^ 1, t ^ 2, t ^ 3, t >> 1, core, 2 + core, 1 - core, 3 - core])
        starts = np.concatenate([[0], np.cumsum(CHUNKS)]).tolist()

        def norm(chunks):
            first = starts[chunks[0]]
            step_rows = 2 if first % 2 == 0 and all(CHUNKS[i] % 2 == 0 for i in chunks) else 1
            plan, specs, shapes = [], [], []
            for i in chunks:
                r0, r1 = starts[i] - first, starts[i + 1] - first
                lo, hi = r0 // step_rows, (r1 - 1) // step_rows
                n = min(step_rows, r1 - r0)
                plan.append((lo, hi, [(r0 + k) % step_rows for k in range(n)]))
                specs.append(pl.BlockSpec((n, width, blk), lambda b, lo=lo, hi=hi: (jnp.clip(b - lo, 0, hi - lo), 0, 0)))
                shapes.append(jax.ShapeDtypeStruct((r1 - r0, width, blk), BF16))
            total = starts[chunks[-1] + 1] - first
            return list(pl.pallas_call(
                functools.partial(norm_kernel, plan),
                grid=(total // step_rows,),
                in_specs=[pl.BlockSpec((step_rows, blk, width), lambda b: (first // step_rows + b, 0, 0)),
                          pl.BlockSpec((width,), lambda b: (0,)),
                          pl.BlockSpec((width,), lambda b: (0,))],
                out_specs=specs,
                out_shape=shapes,
                compiler_params=params(60),
                cost_estimate=pl.CostEstimate(flops=total * 500_000_000, bytes_accessed=total * 800_000, transcendentals=0),
                name="norm",
            )(hidden, ln_gamma, ln_beta))

        a_own = norm([0])
        a_own += norm(list(range(1, len(CHUNKS))))
        a_x = []
        for a in a_own:
            a_x.append(lax.ppermute(a, 'sp', across_x))
        a_c = []
        for a in a_own:
            a_c.append(lax.ppermute(a, 'sp', across_core))

        last = pos_ids[:, blk - 1:].reshape(1, n_rows)
        last_x = lax.ppermute(last, 'sp', across_x)
        last_c = lax.ppermute(last, 'sp', across_core)
        last_xc = lax.ppermute(last_x, 'sp', across_core)
        mask_pos = jnp.where(t == 3, last, jnp.where(t == 2, last_c, jnp.where(t == 1, last_x, last_xc)))[0]
        freq = jnp.asarray(inv_freq.astype(np.float32))
        angle = jnp.stack([mask_pos, ctx_len - 1], axis=1).astype(F32)[:, :, None] * freq
        col = jnp.stack([jnp.cos(angle), jnp.sin(angle)], axis=2).reshape(n_rows, 64, 1)
        col = jnp.broadcast_to(col, (n_rows, 64, 128))
        fine = inv_freq[:, None] * np.arange(blk)
        fine_c, fine_s = np.cos(fine).astype(np.float32)[None], np.sin(fine).astype(np.float32)[None]
        coarse = inv_freq[None, :, None] * (np.arange(4) * blk)[:, None, None]
        coarse_c, coarse_s = np.cos(coarse).astype(np.float32), np.sin(coarse).astype(np.float32)
        tab = jnp.concatenate([fine_c * jnp.asarray(coarse_c) - fine_s * jnp.asarray(coarse_s),
                               fine_s * jnp.asarray(coarse_c) + fine_c * jnp.asarray(coarse_s)], axis=1)

        bias = b_qkv.transpose(1, 0, 2).reshape(3, 2, 2, half)
        bias = lax.dynamic_index_in_dim(bias, core, 2, keepdims=False).reshape(3 * rows, 1)
        bias = jnp.broadcast_to(bias.astype(F32), (3 * rows, 128))
        w, bias, col, tab = lax.optimization_barrier((w_qkv, bias, col, tab))
        w = w.transpose(2, 1, 3, 0).reshape(3, 2, 2, half, width)
        w = lax.dynamic_index_in_dim(w, core, 2, keepdims=False).reshape(3 * rows, width)
        wd = w_dense.reshape(4, half, width)

        row_of = [jnp.full((1,), r, jnp.int32) for r in starts[:-1]]

        keys = values = out = None

        def finish(item, out):
            i, own, other = item
            n = CHUNKS[i]
            extra = [] if out is None else [out]
            return pl.pallas_call(
                dense_kernel,
                grid_spec=pltpu.PrefetchScalarGridSpec(
                    num_scalar_prefetch=2,
                    grid=(n,),
                    in_specs=[pl.BlockSpec((1, blk, rows), lambda b, s, r: (b, 0, 0)),
                              pl.BlockSpec((1, blk, rows), lambda b, s, r: (b, 0, 0)),
                              pl.BlockSpec((1, width, blk), lambda b, s, r: (b, 0, 0))]
                    + [pl.BlockSpec((1, half, width), lambda b, s, r, k=k: (s[k], 0, 0)) for k in (5, 6, 7, 8)]
                    + [pl.BlockSpec((width,), lambda b, s, r: (0,))]
                    + [pl.BlockSpec(memory_space=pl.ANY)] * len(extra),
                    out_specs=pl.BlockSpec((1, blk, width), lambda b, s, r: (r[0] + b, 0, 0)),
                ),
                out_shape=jax.ShapeDtypeStruct((n_rows, blk, width), BF16),
                input_output_aliases={10: 0} if extra else {},
                compiler_params=params(24),
                cost_estimate=pl.CostEstimate(flops=n * 1_000_000_000, bytes_accessed=n * 2_000_000, transcendentals=0),
                name="dense",
            )(idx, row_of[i], own, other, a_own[i], wd, wd, wd, wd, b_dense, *extra)

        a_xc = {}

        def fetch(i, after):
            got = lax.optimization_barrier((a_x[i], *after))
            a_xc[i] = lax.ppermute(got[0], 'sp', across_core)

        fetch(0, (a_own[1], w, bias, col))
        pending = []
        for i, n in enumerate(CHUNKS):
            extra = [] if keys is None else [keys, values]
            a_spec = pl.BlockSpec((1, width, blk), lambda b, *_: (b, 0, 0))
            kv_shape = jax.ShapeDtypeStruct((n_rows, half, 4 * blk), BF16)
            kv_spec = pl.BlockSpec((1, half, 4 * blk), lambda b, i, c, r: (r[0] + b, 0, 0))
            c_shape = jax.ShapeDtypeStruct((n, blk, rows), BF16)
            c_spec = pl.BlockSpec((1, blk, rows), lambda b, *_: (b, 0, 0))
            attn = pl.pallas_call(
                functools.partial(attn_kernel, heads),
                grid_spec=pltpu.PrefetchScalarGridSpec(
                    num_scalar_prefetch=3,
                    grid=(n,),
                    in_specs=[a_spec] * 4 + [
                        pl.BlockSpec((4, 32, blk), lambda b, *_: (0, 0, 0)),
                        pl.BlockSpec((1, 64, 128), lambda b, i, c, r: (r[0] + b, 0, 0)),
                        pl.BlockSpec((3 * rows, width), lambda b, *_: (0, 0)),
                        pl.BlockSpec((3 * rows, 128), lambda b, *_: (0, 0))]
                    + [pl.BlockSpec(memory_space=pl.ANY)] * len(extra),
                    out_specs=[kv_spec, kv_spec, c_spec, c_spec],
                    scratch_shapes=[
                        pltpu.VMEM((4, heads // 2, blk, 128), BF16),
                        pltpu.VMEM((4, rows, blk), BF16),
                        pltpu.VMEM((4, rows, blk), BF16),
                        pltpu.VMEM((2, heads, 128, blk), BF16),
                        pltpu.VMEM((2, 4 * blk, blk), F32),
                        pltpu.VMEM((2, 4 * blk, blk), BF16),
                        pltpu.VMEM((2, rows, blk), BF16),
                        pltpu.VMEM((2, blk, blk), F32),
                    ],
                ),
                out_shape=[kv_shape, kv_shape, c_shape, c_shape],
                input_output_aliases={11: 0, 12: 1} if extra else {},
                compiler_params=params(28),
                cost_estimate=pl.CostEstimate(flops=n * 6_000_000_000, bytes_accessed=n * 4_000_000, transcendentals=0),
                name="attn",
            )
            keys, values, own, send = attn(idx, ctx_len, row_of[i], a_own[i], a_c[i], a_x[i], a_xc[i], tab, col, w, bias, *extra)
            other = lax.ppermute(send, 'sp', across_core)
            if i + 1 < len(CHUNKS):
                fetch(i + 1, (own,) + (() if out is None else (out,)))
            for item in pending:
                out = finish(item, out)
            pending = [(i, own, other)]
        for item in pending:
            out = finish(item, out)

        def by_heads(x):
            return x.reshape(n_rows, n_heads // 4, hd, 4 * blk).transpose(0, 3, 1, 2)

        return out, by_heads(keys), by_heads(values)

    return jax.shard_map(local_block, mesh=mesh, in_specs=(seq_spec, row_spec, row_spec, P('dp'), replicated, replicated, replicated, replicated, replicated, replicated), out_specs=(seq_spec, head_spec, head_spec), check_vma=False)
```

```python
import functools
import math
import numpy as np
import jax
import jax.numpy as jnp
from jax import lax
from jax.experimental import pallas as pl
from jax.experimental.pallas import tpu as pltpu
from jax.sharding import PartitionSpec as P

ALPHA = math.sqrt(56.0)
ROPE_BASE = 10000.0
LN_EPS = 1e-5
LOG2E = 1.4426950408889634
CHUNKS = (4, 3, 3, 3, 3)
F32 = jnp.float32
BF16 = jnp.bfloat16


def mm(a, b):
    return jnp.dot(a, b, preferred_element_type=F32)


def row_vector(ref):
    return ref[...].astype(F32).reshape(1, ref.shape[0])


def norm_kernel(plan, h_ref, g_ref, b_ref, *o_refs):
    def row(r):
        x = h_ref[r].astype(F32)
        x = x - jnp.mean(x, axis=-1, keepdims=True)
        var = jnp.mean(x * x, axis=-1, keepdims=True)
        y = x * lax.rsqrt(var + LN_EPS) * row_vector(g_ref) + row_vector(b_ref)
        return y.astype(BF16).T

    out = [row(r) for r in range(h_ref.shape[0])]
    step = pl.program_id(0)
    for (lo, hi, rows), o_ref in zip(plan, o_refs):
        @pl.when((step >= lo) & (step <= hi))
        def _():
            for i, r in enumerate(rows):
                o_ref[i] = out[r]


def rotate(x, cos_a, sin_a, cos_b, sin_b):
    u0, w0, u1, w1 = (x[16 * i:16 * i + 16] for i in range(4))
    parts = [u0 * cos_a - w0 * sin_a, w0 * cos_a + u0 * sin_a,
             u1 * cos_b - w1 * sin_b, w1 * cos_b + u1 * sin_b]
    return jnp.concatenate(parts, axis=0).astype(BF16)


def fold(accs, x, op):
    accs = list(accs) if accs else [None] * 4
    for i in range(x.shape[0] // 8):
        v = x[8 * i:8 * i + 8]
        accs[i % 4] = v if accs[i % 4] is None else op(accs[i % 4], v)
    return accs


def join(accs, op):
    return op(op(accs[0], accs[1]), op(accs[2], accs[3]))


def attn_kernel(heads, idx_ref, ctx_ref, row_ref, a0, a1, a2, a3, tab_ref, col_ref, w_ref, bias_ref, *rest):
    k_out, v_out, c_own, c_send, kn, kt, vt, qt, s_s, p_s, c_s, m_s = rest[-12:]
    hd = 64
    rows = heads * hd
    blk = a0.shape[2]
    ctx = ctx_ref[row_ref[0] + pl.program_id(0)]

    col = [jnp.concatenate([col_ref[0, 16 * i:16 * i + 16]] * 2, axis=1) for i in range(4)]
    for m, a_ref in enumerate((a0, a1, a2, a3)):
        j = idx_ref[m]
        a = a_ref[0]
        cos, sin = tab_ref[j, :16], tab_ref[j, 16:]
        inside = j * blk + lax.broadcasted_iota(jnp.int32, (1, blk), 1) < ctx
        tab = (jnp.where(inside, cos, col[0]), jnp.where(inside, sin, col[1]),
               jnp.where(inside, 1.0, cos * col[2] + sin * col[3]),
               jnp.where(inside, 0.0, sin * col[2] - cos * col[3]))

        def project(part):
            lo = part * rows
            b = bias_ref[lo:lo + rows]
            return (mm(w_ref[lo:lo + rows], a) + jnp.concatenate([b, b], axis=1)).astype(BF16)

        if m < 2:
            q = project(0)
            for h in range(heads):
                qh = rotate(q[h * hd:(h + 1) * hd].astype(F32), *tab)
                zero = jnp.zeros_like(qh)
                qt[m, h] = jnp.concatenate([qh, zero] if h % 2 == 0 else [zero, qh], axis=0)
        k = project(1)
        for p in range(heads // 2):
            pair = [rotate(k[(2 * p + i) * hd:(2 * p + i + 1) * hd].astype(F32), *tab) for i in range(2)]
            pair = jnp.concatenate(pair, axis=0)
            kt[j, p * 128:(p + 1) * 128] = pair
            kn[j, p] = pair.T
        vt[j] = project(2)

    half = rows // 2
    out_lo = pl.multiple_of(idx_ref[4] * half, half)

    def copy_out(j, carry):
        to = pl.ds(pl.multiple_of(j * blk, blk), blk)
        k_out[0, :, to] = kt[j, pl.ds(out_lo, half)]
        v_out[0, :, to] = vt[j, pl.ds(out_lo, half)]
        return carry

    lax.fori_loop(0, 4, copy_out, 0)

    scale = LOG2E / math.sqrt(hd)

    def attend(nb, masked, qi, jq):
        q_pos = jq * blk + lax.broadcasted_iota(jnp.int32, (1, blk), 1)
        limit = jnp.maximum(q_pos, ctx - 1)
        for kb in masked:
            key_pos = kb * blk + lax.broadcasted_iota(jnp.int32, (blk, blk), 0)
            m_s[kb % 2] = jnp.where(key_pos <= limit, 0.0, -jnp.inf)
        top, total, acc = {}, {}, {}
        for step in range(heads + 2):
            h0, h1, h2 = step, step - 1, step - 2
            if 0 <= h1 < heads:
                top[h1] = jnp.max(join(top[h1], jnp.maximum), axis=0, keepdims=True)
            for kb in range(nb):
                lo = kb * blk
                if h0 < heads:
                    s = mm(kn[kb, h0 // 2], qt[qi, h0])
                    if kb in masked:
                        s = s + m_s[kb % 2]
                    s_s[h0 % 2, lo:lo + blk] = s
                    top[h0] = fold(top.get(h0), s, jnp.maximum)
                if 0 <= h1 < heads:
                    for r in range(lo, lo + blk, 32):
                        e = jnp.exp2((s_s[h1 % 2, r:r + 32] - top[h1]) * scale)
                        total[h1] = fold(total.get(h1), e, jnp.add)
                        p_s[h1 % 2, r:r + 32] = e.astype(BF16)
                if 0 <= h2 < heads:
                    t = mm(vt[kb, h2 * hd:(h2 + 1) * hd], p_s[h2 % 2, lo:lo + blk])
                    acc[h2] = acc[h2] + t if kb else t
            if 0 <= h2 < heads:
                t = jnp.sum(join(total[h2], jnp.add), axis=0, keepdims=True)
                c_s[qi, h2 * hd:(h2 + 1) * hd] = (acc[h2] / t).astype(BF16)

    def query_block(qi, carry):
        jq = idx_ref[qi]
        pl.when(jq < 3)(functools.partial(attend, 3, (1, 2), qi, jq))
        pl.when(jq == 3)(functools.partial(attend, 4, (3,), qi, jq))
        return carry

    lax.fori_loop(0, 2, query_block, 0)
    c_own[0] = c_s[0].T
    c_send[0] = c_s[1].T


def dense_kernel(idx_ref, row_ref, own_ref, other_ref, a_ref, w0, w1, w2, w3, b_ref, *rest):
    o_ref = rest[-1]
    for r in range(o_ref.shape[0]):
        w = jnp.concatenate([w0[0], w1[0]], axis=0)
        acc = mm(own_ref[r], w)
        w = jnp.concatenate([w2[0], w3[0]], axis=0)
        acc = acc + mm(other_ref[r], w)
        o_ref[r] = (a_ref[r].T.astype(F32) * ALPHA + (acc + row_vector(b_ref))).astype(BF16)


def params(mib):
    return pltpu.CompilerParams(dimension_semantics=("arbitrary",), vmem_limit_bytes=mib * 1024 * 1024)


def solution(mesh):
    seq_spec = P('dp', 'sp', None)
    row_spec = P('dp', 'sp')
    head_spec = P('dp', None, 'sp', None)
    replicated = P()
    across_x = [(i, i ^ 2) for i in range(4)]
    across_core = [(i, i ^ 1) for i in range(4)]
    inv_freq = ROPE_BASE ** (-np.arange(0, 32, 2, dtype=np.float64) / 32)

    def local_block(hidden, pos_ids, block_ids, ctx_len, ln_gamma, ln_beta, w_qkv, b_qkv, w_dense, b_dense):
        n_rows, blk, width = hidden.shape
        n_heads, _, hd = b_qkv.shape
        heads = n_heads // 2
        rows = heads * hd
        half = rows // 2
        t = lax.axis_index('sp').astype(jnp.int32)
        core = t & 1
        idx = jnp.stack([t, t ^ 1, t ^ 2, t ^ 3, t >> 1, core, 2 + core, 1 - core, 3 - core])
        starts = np.concatenate([[0], np.cumsum(CHUNKS)]).tolist()

        def norm(chunks):
            first = starts[chunks[0]]
            step_rows = 2 if first % 2 == 0 and all(CHUNKS[i] % 2 == 0 for i in chunks) else 1
            plan, specs, shapes = [], [], []
            for i in chunks:
                r0, r1 = starts[i] - first, starts[i + 1] - first
                lo, hi = r0 // step_rows, (r1 - 1) // step_rows
                n = min(step_rows, r1 - r0)
                plan.append((lo, hi, [(r0 + k) % step_rows for k in range(n)]))
                specs.append(pl.BlockSpec((n, width, blk), lambda b, lo=lo, hi=hi: (jnp.clip(b - lo, 0, hi - lo), 0, 0)))
                shapes.append(jax.ShapeDtypeStruct((r1 - r0, width, blk), BF16))
            total = starts[chunks[-1] + 1] - first
            return list(pl.pallas_call(
                functools.partial(norm_kernel, plan),
                grid=(total // step_rows,),
                in_specs=[pl.BlockSpec((step_rows, blk, width), lambda b: (first // step_rows + b, 0, 0)),
                          pl.BlockSpec((width,), lambda b: (0,)),
                          pl.BlockSpec((width,), lambda b: (0,))],
                out_specs=specs,
                out_shape=shapes,
                compiler_params=params(60),
                cost_estimate=pl.CostEstimate(flops=total * 500_000_000, bytes_accessed=total * 800_000, transcendentals=0),
                name="norm",
            )(hidden, ln_gamma, ln_beta))

        a_own = norm([0])
        a_own += norm(list(range(1, len(CHUNKS))))
        a_x = []
        for a in a_own:
            a_x.append(lax.ppermute(a, 'sp', across_x))
        a_c = []
        for a in a_own:
            a_c.append(lax.ppermute(a, 'sp', across_core))

        pos_ids, _ = lax.optimization_barrier((pos_ids, a_own[0]))
        last = pos_ids[:, blk - 1:].reshape(1, n_rows)
        last_x = lax.ppermute(last, 'sp', across_x)
        last_c = lax.ppermute(last, 'sp', across_core)
        last_xc = lax.ppermute(last_x, 'sp', across_core)
        mask_pos = jnp.where(t == 3, last, jnp.where(t == 2, last_c, jnp.where(t == 1, last_x, last_xc)))[0]
        freq = jnp.asarray(inv_freq.astype(np.float32))
        angle = jnp.stack([mask_pos, ctx_len - 1], axis=1).astype(F32)[:, :, None] * freq
        col = jnp.stack([jnp.cos(angle), jnp.sin(angle)], axis=2).reshape(n_rows, 64, 1)
        col = jnp.broadcast_to(col, (n_rows, 64, 128))
        fine = inv_freq[:, None] * np.arange(blk)
        fine_c, fine_s = np.cos(fine).astype(np.float32)[None], np.sin(fine).astype(np.float32)[None]
        coarse = inv_freq[None, :, None] * (np.arange(4) * blk)[:, None, None]
        coarse_c, coarse_s = np.cos(coarse).astype(np.float32), np.sin(coarse).astype(np.float32)
        tab = jnp.concatenate([fine_c * jnp.asarray(coarse_c) - fine_s * jnp.asarray(coarse_s),
                               fine_s * jnp.asarray(coarse_c) + fine_c * jnp.asarray(coarse_s)], axis=1)

        bias = b_qkv.transpose(1, 0, 2).reshape(3, 2, 2, half)
        bias = lax.dynamic_index_in_dim(bias, core, 2, keepdims=False).reshape(3 * rows, 1)
        bias = jnp.broadcast_to(bias.astype(F32), (3 * rows, 128))
        w, bias, col, tab = lax.optimization_barrier((w_qkv, bias, col, tab))
        w = w.transpose(2, 1, 3, 0).reshape(3, 2, 2, half, width)
        w = lax.dynamic_index_in_dim(w, core, 2, keepdims=False).reshape(3 * rows, width)
        wd = w_dense.reshape(4, half, width)

        row_of = [jnp.full((1,), r, jnp.int32) for r in starts[:-1]]

        keys = values = out = None

        def finish(item, out):
            i, own, other = item
            n = CHUNKS[i]
            extra = [] if out is None else [out]
            return pl.pallas_call(
                dense_kernel,
                grid_spec=pltpu.PrefetchScalarGridSpec(
                    num_scalar_prefetch=2,
                    grid=(n,),
                    in_specs=[pl.BlockSpec((1, blk, rows), lambda b, s, r: (b, 0, 0)),
                              pl.BlockSpec((1, blk, rows), lambda b, s, r: (b, 0, 0)),
                              pl.BlockSpec((1, width, blk), lambda b, s, r: (b, 0, 0))]
                    + [pl.BlockSpec((1, half, width), lambda b, s, r, k=k: (s[k], 0, 0)) for k in (5, 6, 7, 8)]
                    + [pl.BlockSpec((width,), lambda b, s, r: (0,))]
                    + [pl.BlockSpec(memory_space=pl.ANY)] * len(extra),
                    out_specs=pl.BlockSpec((1, blk, width), lambda b, s, r: (r[0] + b, 0, 0)),
                ),
                out_shape=jax.ShapeDtypeStruct((n_rows, blk, width), BF16),
                input_output_aliases={10: 0} if extra else {},
                compiler_params=params(24),
                cost_estimate=pl.CostEstimate(flops=n * 1_000_000_000, bytes_accessed=n * 2_000_000, transcendentals=0),
                name="dense",
            )(idx, row_of[i], own, other, a_own[i], wd, wd, wd, wd, b_dense, *extra)

        a_xc = {}

        def fetch(i, after):
            got = lax.optimization_barrier((a_x[i], *after))
            a_xc[i] = lax.ppermute(got[0], 'sp', across_core)

        fetch(0, (a_own[1], w, bias, col))
        pending = []
        for i, n in enumerate(CHUNKS):
            extra = [] if keys is None else [keys, values]
            a_spec = pl.BlockSpec((1, width, blk), lambda b, *_: (b, 0, 0))
            kv_shape = jax.ShapeDtypeStruct((n_rows, half, 4 * blk), BF16)
            kv_spec = pl.BlockSpec((1, half, 4 * blk), lambda b, i, c, r: (r[0] + b, 0, 0))
            c_shape = jax.ShapeDtypeStruct((n, blk, rows), BF16)
            c_spec = pl.BlockSpec((1, blk, rows), lambda b, *_: (b, 0, 0))
            attn = pl.pallas_call(
                functools.partial(attn_kernel, heads),
                grid_spec=pltpu.PrefetchScalarGridSpec(
                    num_scalar_prefetch=3,
                    grid=(n,),
                    in_specs=[a_spec] * 4 + [
                        pl.BlockSpec((4, 32, blk), lambda b, *_: (0, 0, 0)),
                        pl.BlockSpec((1, 64, 128), lambda b, i, c, r: (r[0] + b, 0, 0)),
                        pl.BlockSpec((3 * rows, width), lambda b, *_: (0, 0)),
                        pl.BlockSpec((3 * rows, 128), lambda b, *_: (0, 0))]
                    + [pl.BlockSpec(memory_space=pl.ANY)] * len(extra),
                    out_specs=[kv_spec, kv_spec, c_spec, c_spec],
                    scratch_shapes=[
                        pltpu.VMEM((4, heads // 2, blk, 128), BF16),
                        pltpu.VMEM((4, rows, blk), BF16),
                        pltpu.VMEM((4, rows, blk), BF16),
                        pltpu.VMEM((2, heads, 128, blk), BF16),
                        pltpu.VMEM((2, 4 * blk, blk), F32),
                        pltpu.VMEM((2, 4 * blk, blk), BF16),
                        pltpu.VMEM((2, rows, blk), BF16),
                        pltpu.VMEM((2, blk, blk), F32),
                    ],
                ),
                out_shape=[kv_shape, kv_shape, c_shape, c_shape],
                input_output_aliases={11: 0, 12: 1} if extra else {},
                compiler_params=params(22),
                cost_estimate=pl.CostEstimate(flops=n * 6_000_000_000, bytes_accessed=n * 4_000_000, transcendentals=0),
                name="attn",
            )
            keys, values, own, send = attn(idx, ctx_len, row_of[i], a_own[i], a_c[i], a_x[i], a_xc[i], tab, col, w, bias, *extra)
            other = lax.ppermute(send, 'sp', across_core)
            if i + 1 < len(CHUNKS):
                fetch(i + 1, (own,) + (() if out is None else (out,)))
            for item in pending:
                out = finish(item, out)
            pending = [(i, own, other)]
        for item in pending:
            out = finish(item, out)

        def by_heads(x):
            return x.reshape(n_rows, n_heads // 4, hd, 4 * blk).transpose(0, 3, 1, 2)

        return out, by_heads(keys), by_heads(values)

    return jax.shard_map(local_block, mesh=mesh, in_specs=(seq_spec, row_spec, row_spec, P('dp'), replicated, replicated, replicated, replicated, replicated, replicated), out_specs=(seq_spec, head_spec, head_spec), check_vma=False)
```

```python
import functools
import math
import numpy as np
import jax
import jax.numpy as jnp
from jax import lax
from jax.experimental import pallas as pl
from jax.experimental.pallas import tpu as pltpu
from jax.sharding import PartitionSpec as P

ALPHA = math.sqrt(56.0)
ROPE_BASE = 10000.0
LN_EPS = 1e-5
LOG2E = 1.4426950408889634
CHUNKS = (4, 4, 3, 3, 2)
F32 = jnp.float32
BF16 = jnp.bfloat16


def mm(a, b):
    return jnp.dot(a, b, preferred_element_type=F32)


def row_vector(ref):
    return ref[...].astype(F32).reshape(1, ref.shape[0])


def norm_kernel(plan, h_ref, g_ref, b_ref, *o_refs):
    def row(r):
        x = h_ref[r].astype(F32)
        x = x - jnp.mean(x, axis=-1, keepdims=True)
        var = jnp.mean(x * x, axis=-1, keepdims=True)
        y = x * lax.rsqrt(var + LN_EPS) * row_vector(g_ref) + row_vector(b_ref)
        return y.astype(BF16).T

    out = [row(r) for r in range(h_ref.shape[0])]
    step = pl.program_id(0)
    for (lo, hi, rows), o_ref in zip(plan, o_refs):
        @pl.when((step >= lo) & (step <= hi))
        def _():
            for i, r in enumerate(rows):
                o_ref[i] = out[r]


def rotate(x, cos_a, sin_a, cos_b, sin_b):
    u0, w0, u1, w1 = (x[16 * i:16 * i + 16] for i in range(4))
    parts = [u0 * cos_a - w0 * sin_a, w0 * cos_a + u0 * sin_a,
             u1 * cos_b - w1 * sin_b, w1 * cos_b + u1 * sin_b]
    return jnp.concatenate(parts, axis=0).astype(BF16)


def fold(accs, x, op):
    accs = list(accs) if accs else [None] * 4
    for i in range(x.shape[0] // 8):
        v = x[8 * i:8 * i + 8]
        accs[i % 4] = v if accs[i % 4] is None else op(accs[i % 4], v)
    return accs


def join(accs, op):
    return op(op(accs[0], accs[1]), op(accs[2], accs[3]))


def attn_kernel(heads, idx_ref, ctx_ref, row_ref, a0, a1, a2, a3, tab_ref, col_ref, w_ref, bias_ref, *rest):
    k_out, v_out, c_own, c_send, kn, kt, vt, qt, s_s, p_s, c_s, m_s = rest[-12:]
    hd = 64
    rows = heads * hd
    blk = a0.shape[2]
    ctx = ctx_ref[row_ref[0] + pl.program_id(0)]

    col = [jnp.concatenate([col_ref[16 * i:16 * i + 16]] * 2, axis=1) for i in range(4)]
    for m, a_ref in enumerate((a0, a1, a2, a3)):
        j = idx_ref[m]
        a = a_ref[0]
        cos, sin = tab_ref[j, :16], tab_ref[j, 16:]
        inside = j * blk + lax.broadcasted_iota(jnp.int32, (1, blk), 1) < ctx
        tab = (jnp.where(inside, cos, col[0]), jnp.where(inside, sin, col[1]),
               jnp.where(inside, 1.0, cos * col[2] + sin * col[3]),
               jnp.where(inside, 0.0, sin * col[2] - cos * col[3]))

        def project(part):
            lo = part * rows
            b = bias_ref[lo:lo + rows]
            return (mm(w_ref[lo:lo + rows], a) + jnp.concatenate([b, b], axis=1)).astype(BF16)

        if m < 2:
            q = project(0)
            for h in range(heads):
                qh = rotate(q[h * hd:(h + 1) * hd].astype(F32), *tab)
                zero = jnp.zeros_like(qh)
                qt[m, h] = jnp.concatenate([qh, zero] if h % 2 == 0 else [zero, qh], axis=0)
        k = project(1)
        for p in range(heads // 2):
            pair = [rotate(k[(2 * p + i) * hd:(2 * p + i + 1) * hd].astype(F32), *tab) for i in range(2)]
            pair = jnp.concatenate(pair, axis=0)
            kt[j, p * 128:(p + 1) * 128] = pair
            kn[j, p] = pair.T
        vt[j] = project(2)

    half = rows // 2
    out_lo = pl.multiple_of(idx_ref[4] * half, half)

    def copy_out(j, carry):
        to = pl.ds(pl.multiple_of(j * blk, blk), blk)
        k_out[0, :, to] = kt[j, pl.ds(out_lo, half)]
        v_out[0, :, to] = vt[j, pl.ds(out_lo, half)]
        return carry

    lax.fori_loop(0, 4, copy_out, 0)

    scale = LOG2E / math.sqrt(hd)

    def attend(nb, masked, qi, jq):
        q_pos = jq * blk + lax.broadcasted_iota(jnp.int32, (1, blk), 1)
        limit = jnp.maximum(q_pos, ctx - 1)
        for kb in masked:
            key_pos = kb * blk + lax.broadcasted_iota(jnp.int32, (blk, blk), 0)
            m_s[kb % 2] = jnp.where(key_pos <= limit, 0.0, -jnp.inf)
        top, total, acc = {}, {}, {}
        for step in range(heads + 2):
            h0, h1, h2 = step, step - 1, step - 2
            if 0 <= h1 < heads:
                top[h1] = jnp.max(join(top[h1], jnp.maximum), axis=0, keepdims=True)
            for kb in range(nb):
                lo = kb * blk
                if h0 < heads:
                    s = mm(kn[kb, h0 // 2], qt[qi, h0])
                    if kb in masked:
                        s = s + m_s[kb % 2]
                    s_s[h0 % 2, lo:lo + blk] = s
                    top[h0] = fold(top.get(h0), s, jnp.maximum)
                if 0 <= h1 < heads:
                    for r in range(lo, lo + blk, 32):
                        e = jnp.exp2((s_s[h1 % 2, r:r + 32] - top[h1]) * scale)
                        total[h1] = fold(total.get(h1), e, jnp.add)
                        p_s[h1 % 2, r:r + 32] = e.astype(BF16)
                if 0 <= h2 < heads:
                    t = mm(vt[kb, h2 * hd:(h2 + 1) * hd], p_s[h2 % 2, lo:lo + blk])
                    acc[h2] = acc[h2] + t if kb else t
            if 0 <= h2 < heads:
                t = jnp.sum(join(total[h2], jnp.add), axis=0, keepdims=True)
                c_s[qi, h2 * hd:(h2 + 1) * hd] = (acc[h2] / t).astype(BF16)

    def query_block(qi, carry):
        jq = idx_ref[qi]
        pl.when(jq < 3)(functools.partial(attend, 3, (1, 2), qi, jq))
        pl.when(jq == 3)(functools.partial(attend, 4, (3,), qi, jq))
        return carry

    lax.fori_loop(0, 2, query_block, 0)
    c_own[0] = c_s[0].T
    c_send[0] = c_s[1].T


def dense_kernel(idx_ref, row_ref, own_ref, other_ref, a_ref, w0, w1, w2, w3, b_ref, *rest):
    o_ref = rest[-1]
    for r in range(o_ref.shape[0]):
        w = jnp.concatenate([w0[0], w1[0]], axis=0)
        acc = mm(own_ref[r], w)
        w = jnp.concatenate([w2[0], w3[0]], axis=0)
        acc = acc + mm(other_ref[r], w)
        o_ref[r] = (a_ref[r].T.astype(F32) * ALPHA + (acc + row_vector(b_ref))).astype(BF16)


def params(mib):
    return pltpu.CompilerParams(dimension_semantics=("arbitrary",), vmem_limit_bytes=mib * 1024 * 1024)


def solution(mesh):
    seq_spec = P('dp', 'sp', None)
    row_spec = P('dp', 'sp')
    head_spec = P('dp', None, 'sp', None)
    replicated = P()
    across_x = [(i, i ^ 2) for i in range(4)]
    across_core = [(i, i ^ 1) for i in range(4)]
    inv_freq = ROPE_BASE ** (-np.arange(0, 32, 2, dtype=np.float64) / 32)

    def local_block(hidden, pos_ids, block_ids, ctx_len, ln_gamma, ln_beta, w_qkv, b_qkv, w_dense, b_dense):
        n_rows, blk, width = hidden.shape
        n_heads, _, hd = b_qkv.shape
        heads = n_heads // 2
        rows = heads * hd
        half = rows // 2
        t = lax.axis_index('sp').astype(jnp.int32)
        core = t & 1
        idx = jnp.stack([t, t ^ 1, t ^ 2, t ^ 3, t >> 1, core, 2 + core, 1 - core, 3 - core])
        starts = np.concatenate([[0], np.cumsum(CHUNKS)]).tolist()

        def norm(chunks):
            first = starts[chunks[0]]
            step_rows = 2 if first % 2 == 0 and all(CHUNKS[i] % 2 == 0 for i in chunks) else 1
            plan, specs, shapes = [], [], []
            for i in chunks:
                r0, r1 = starts[i] - first, starts[i + 1] - first
                lo, hi = r0 // step_rows, (r1 - 1) // step_rows
                n = min(step_rows, r1 - r0)
                plan.append((lo, hi, [(r0 + k) % step_rows for k in range(n)]))
                specs.append(pl.BlockSpec((n, width, blk), lambda b, lo=lo, hi=hi: (jnp.clip(b - lo, 0, hi - lo), 0, 0)))
                shapes.append(jax.ShapeDtypeStruct((r1 - r0, width, blk), BF16))
            total = starts[chunks[-1] + 1] - first
            return list(pl.pallas_call(
                functools.partial(norm_kernel, plan),
                grid=(total // step_rows,),
                in_specs=[pl.BlockSpec((step_rows, blk, width), lambda b: (first // step_rows + b, 0, 0)),
                          pl.BlockSpec((width,), lambda b: (0,)),
                          pl.BlockSpec((width,), lambda b: (0,))],
                out_specs=specs,
                out_shape=shapes,
                compiler_params=params(60),
                cost_estimate=pl.CostEstimate(flops=total * 500_000_000, bytes_accessed=total * 800_000, transcendentals=0),
                name="norm",
            )(hidden, ln_gamma, ln_beta))

        a_own = norm([0])
        a_own += norm(list(range(1, len(CHUNKS))))
        a_x = []
        for a in a_own:
            a_x.append(lax.ppermute(a, 'sp', across_x))
        a_c = []
        for a in a_own:
            a_c.append(lax.ppermute(a, 'sp', across_core))

        pos_ids, _ = lax.optimization_barrier((pos_ids, a_own[0]))
        last = pos_ids[:, blk - 1:].reshape(1, n_rows)
        last_x = lax.ppermute(last, 'sp', across_x)
        last_c = lax.ppermute(last, 'sp', across_core)
        last_xc = lax.ppermute(last_x, 'sp', across_core)
        mask_pos = jnp.where(t == 3, last, jnp.where(t == 2, last_c, jnp.where(t == 1, last_x, last_xc)))[0]
        freq = jnp.asarray(inv_freq.astype(np.float32))
        angle = jnp.stack([mask_pos, ctx_len - 1], axis=1).astype(F32)[:, :, None] * freq
        col = jnp.stack([jnp.cos(angle), jnp.sin(angle)], axis=2).reshape(n_rows, 64, 1)
        col = jnp.broadcast_to(col, (n_rows, 64, 128))
        fine = inv_freq[:, None] * np.arange(blk)
        fine_c, fine_s = np.cos(fine).astype(np.float32)[None], np.sin(fine).astype(np.float32)[None]
        coarse = inv_freq[None, :, None] * (np.arange(4) * blk)[:, None, None]
        coarse_c, coarse_s = np.cos(coarse).astype(np.float32), np.sin(coarse).astype(np.float32)
        tab = jnp.concatenate([fine_c * jnp.asarray(coarse_c) - fine_s * jnp.asarray(coarse_s),
                               fine_s * jnp.asarray(coarse_c) + fine_c * jnp.asarray(coarse_s)], axis=1)

        bias = b_qkv.transpose(1, 0, 2).reshape(3, 2, 2, half)
        bias = lax.dynamic_index_in_dim(bias, core, 2, keepdims=False).reshape(3 * rows, 1)
        bias = jnp.broadcast_to(bias.astype(F32), (3 * rows, 128))
        aux = jnp.concatenate([bias, col.reshape(n_rows * 64, 128)], axis=0)
        w, aux, tab = lax.optimization_barrier((w_qkv, aux, tab))
        w = w.transpose(2, 1, 3, 0).reshape(3, 2, 2, half, width)
        w = lax.dynamic_index_in_dim(w, core, 2, keepdims=False).reshape(3 * rows, width)
        wd = w_dense.reshape(4, half, width)

        row_of = [jnp.full((1,), r, jnp.int32) for r in starts[:-1]]

        keys = values = out = None

        def finish(item, out):
            i, own, other = item
            n = CHUNKS[i]
            extra = [] if out is None else [out]
            return pl.pallas_call(
                dense_kernel,
                grid_spec=pltpu.PrefetchScalarGridSpec(
                    num_scalar_prefetch=2,
                    grid=(n,),
                    in_specs=[pl.BlockSpec((1, blk, rows), lambda b, s, r: (b, 0, 0)),
                              pl.BlockSpec((1, blk, rows), lambda b, s, r: (b, 0, 0)),
                              pl.BlockSpec((1, width, blk), lambda b, s, r: (b, 0, 0))]
                    + [pl.BlockSpec((1, half, width), lambda b, s, r, k=k: (s[k], 0, 0)) for k in (5, 6, 7, 8)]
                    + [pl.BlockSpec((width,), lambda b, s, r: (0,))]
                    + [pl.BlockSpec(memory_space=pl.ANY)] * len(extra),
                    out_specs=pl.BlockSpec((1, blk, width), lambda b, s, r: (r[0] + b, 0, 0)),
                ),
                out_shape=jax.ShapeDtypeStruct((n_rows, blk, width), BF16),
                input_output_aliases={10: 0} if extra else {},
                compiler_params=params(24),
                cost_estimate=pl.CostEstimate(flops=n * 1_000_000_000, bytes_accessed=n * 2_000_000, transcendentals=0),
                name="dense",
            )(idx, row_of[i], own, other, a_own[i], wd, wd, wd, wd, b_dense, *extra)

        a_xc = {}

        def fetch(i, after):
            got = lax.optimization_barrier((a_x[i], *after))
            a_xc[i] = lax.ppermute(got[0], 'sp', across_core)

        fetch(0, (a_own[1], w, aux))
        pending = []
        for i, n in enumerate(CHUNKS):
            extra = [] if keys is None else [keys, values]
            a_spec = pl.BlockSpec((1, width, blk), lambda b, *_: (b, 0, 0))
            kv_shape = jax.ShapeDtypeStruct((n_rows, half, 4 * blk), BF16)
            kv_spec = pl.BlockSpec((1, half, 4 * blk), lambda b, i, c, r: (r[0] + b, 0, 0))
            c_shape = jax.ShapeDtypeStruct((n, blk, rows), BF16)
            c_spec = pl.BlockSpec((1, blk, rows), lambda b, *_: (b, 0, 0))
            attn = pl.pallas_call(
                functools.partial(attn_kernel, heads),
                grid_spec=pltpu.PrefetchScalarGridSpec(
                    num_scalar_prefetch=3,
                    grid=(n,),
                    in_specs=[a_spec] * 4 + [
                        pl.BlockSpec((4, 32, blk), lambda b, *_: (0, 0, 0)),
                        pl.BlockSpec((64, 128), lambda b, i, c, r: (3 * rows // 64 + r[0] + b, 0)),
                        pl.BlockSpec((3 * rows, width), lambda b, *_: (0, 0)),
                        pl.BlockSpec((3 * rows, 128), lambda b, *_: (0, 0))]
                    + [pl.BlockSpec(memory_space=pl.ANY)] * len(extra),
                    out_specs=[kv_spec, kv_spec, c_spec, c_spec],
                    scratch_shapes=[
                        pltpu.VMEM((4, heads // 2, blk, 128), BF16),
                        pltpu.VMEM((4, rows, blk), BF16),
                        pltpu.VMEM((4, rows, blk), BF16),
                        pltpu.VMEM((2, heads, 128, blk), BF16),
                        pltpu.VMEM((2, 4 * blk, blk), F32),
                        pltpu.VMEM((2, 4 * blk, blk), BF16),
                        pltpu.VMEM((2, rows, blk), BF16),
                        pltpu.VMEM((2, blk, blk), F32),
                    ],
                ),
                out_shape=[kv_shape, kv_shape, c_shape, c_shape],
                input_output_aliases={11: 0, 12: 1} if extra else {},
                compiler_params=params(22),
                cost_estimate=pl.CostEstimate(flops=n * 6_000_000_000, bytes_accessed=n * 4_000_000, transcendentals=0),
                name="attn",
            )
            keys, values, own, send = attn(idx, ctx_len, row_of[i], a_own[i], a_c[i], a_x[i], a_xc[i], tab, aux, w, aux, *extra)
            other = lax.ppermute(send, 'sp', across_core)
            if i + 1 < len(CHUNKS):
                fetch(i + 1, (own,) + (() if out is None else (out,)))
            for item in pending:
                out = finish(item, out)
            pending = [(i, own, other)]
        for item in pending:
            out = finish(item, out)

        def by_heads(x):
            return x.reshape(n_rows, n_heads // 4, hd, 4 * blk).transpose(0, 3, 1, 2)

        return out, by_heads(keys), by_heads(values)

    return jax.shard_map(local_block, mesh=mesh, in_specs=(seq_spec, row_spec, row_spec, P('dp'), replicated, replicated, replicated, replicated, replicated, replicated), out_specs=(seq_spec, head_spec, head_spec), check_vma=False)
```
